32 devices in a mesh: section: 8 (over y, x, core), dp: 4 (over z).
Axes of the slice: x: 2, y: 2, z: 4, core: 2. Of those that a mesh axis runs over, the one named last changes fastest.
Arguments:
- out_pair: float32 [512, 2048], P('dp'), may hold values from -6 to 6
- out_grad: bfloat16 [512, 2048], P('dp'), may hold values from -6 to 6
- f_weight: bfloat16 [8, 1024, 1024], P('section', 'dp'), may hold values from -0.09375 to 0.09375
- g_weight: bfloat16 [8, 1024, 1024], P('section', 'dp'), may hold values from -0.09375 to 0.09375
- gains: float32 [8, 2, 1024], P('section'), may hold values from 0.1 to 1.9
Outputs:
- in_pair: float32 [8, 512, 2048], P('section', 'dp')
- in_grad: bfloat16 [8, 512, 2048], P('section', 'dp')
- f_grad: float32 [8, 1024, 1024], P('section', 'dp')
- g_grad: float32 [8, 1024, 1024], P('section', 'dp')
- gains_grad: float32 [8, 2, 1024], P('section')
The draws below stay inside these ranges and needn't reach their ends.
All inputs are finite; a program needn't handle non-finite values.
Results may differ from the reference program's by a relative error of at most 0.04.
Values may be sent and summed in bfloat16 or wider, within the bound.
A program may use at most 64 MiB of HBM per device.

```python
import jax
import jax.numpy as jnp
from jax import lax

DH = 1024
TOK_DEV = 128
SECTIONS = 8
TOKENS = 512
N_SECTION = 8
N_DP = 4


def steps_of(key, extent, shards, smallest, top_value):
    gain, own = 1.0, jax.random.fold_in(key, 6)
    for dim, parts in shards:
        steps = jnp.exp(jax.random.uniform(jax.random.fold_in(own, dim), (parts,), jnp.float32, smallest / len(shards), top_value / len(shards)))
        gain = gain * jnp.repeat(steps, extent[dim] // parts).reshape([-1 if axis == dim else 1 for axis in range(len(extent))])
    return gain


def centred(key, dims, width, reach, shards=(), kind=jnp.bfloat16):
    result = width * jax.random.normal(key, dims, jnp.float32)
    if shards:
        result = result * steps_of(key, dims, shards, -0.22, 0.18)
    return jnp.clip(result, -reach, reach).astype(kind)


def setup_inputs(seed: int = 0) -> dict:
    seeds = jax.random.split(jax.random.key(seed), 6)
    out_pair = centred(seeds[0], (TOKENS, 2 * DH), 1.0, 6.0, ((0, 4),), jnp.float32)
    out_grad = centred(seeds[1], (TOKENS, 2 * DH), 1.0, 6.0, ((0, 4),))
    f_weight = centred(seeds[2], (SECTIONS, DH, DH), (4 * DH) ** -0.5, 0.09375, ((0, 8), (1, 4)))
    g_weight = centred(seeds[3], (SECTIONS, DH, DH), (4 * DH) ** -0.5, 0.09375, ((0, 8), (1, 4)))
    gains = jnp.clip(1.0 + 0.18 * jax.random.normal(seeds[4], (SECTIONS, 2, DH), jnp.float32), 0.1, 1.9)
    return {"out_pair": out_pair, "out_grad": out_grad, "f_weight": f_weight, "g_weight": g_weight, "gains": gains}


offset = 0.25

def silu_parts(pre_values):
    sigmoid_value = jax.nn.sigmoid(pre_values)
    return (pre_values * sigmoid_value, sigmoid_value * (1.0 + pre_values * (1.0 - sigmoid_value)))

def normalize(values, gain_row):
    inv_scale = lax.rsqrt(lax.optimization_barrier(jnp.mean(values * values, axis=-1, keepdims=True)) + offset)
    return ((values * inv_scale * gain_row).astype(jnp.bfloat16), inv_scale)

def norm_back(values, inv_scale, gain_row, upstream):
    weighted = gain_row * upstream
    cubed = inv_scale * inv_scale * inv_scale
    return inv_scale * weighted - values * cubed * lax.optimization_barrier(jnp.mean(weighted * values, axis=-1, keepdims=True))

def coupling_back(upper_out, lower_out, upper_grad, lower_grad, w_first, w_second, gain_pair):
    normed_second, scale_second = normalize(upper_out, gain_pair[1])
    pre_second = jnp.dot(normed_second, w_second, preferred_element_type=jnp.float32)
    act_second, slope_second = silu_parts(pre_second)
    lower_in = lower_out - act_second
    normed_first, scale_first = normalize(lower_in, gain_pair[0])
    pre_first = jnp.dot(normed_first, w_first, preferred_element_type=jnp.float32)
    act_first, slope_first = silu_parts(pre_first)
    upper_in = upper_out - act_first
    delta_second = (lower_grad * slope_second).astype(jnp.bfloat16)
    back_second = jnp.dot(delta_second, w_second.T, preferred_element_type=jnp.float32)
    through = upper_grad + norm_back(upper_out, scale_second, gain_pair[1], back_second)
    delta_first = (through * slope_first).astype(jnp.bfloat16)
    back_first = jnp.dot(delta_first, w_first.T, preferred_element_type=jnp.float32)
    lower_total = lower_grad + norm_back(lower_in, scale_first, gain_pair[0], back_first)
    gain_terms = jnp.stack([lax.optimization_barrier(jnp.sum(back_first * lower_in * scale_first, axis=0)), lax.optimization_barrier(jnp.sum(back_second * upper_out * scale_second, axis=0))])
    return (upper_in, lower_in, through.astype(jnp.bfloat16), lower_total.astype(jnp.bfloat16), normed_first, delta_first, normed_second, delta_second, gain_terms)

def replica_sum(normed, delta):
    left_side = normed.reshape(N_DP, TOK_DEV, -1).astype(jnp.float32)
    right_side = delta.reshape(N_DP, TOK_DEV, -1).astype(jnp.float32)
    partial_sums = jnp.einsum('rtd,rte->rde', left_side, right_side)
    rounded = lax.optimization_barrier(partial_sums.astype(jnp.bfloat16))
    return lax.optimization_barrier(jnp.sum(rounded.astype(jnp.float32), axis=0))

def reference(out_pair, out_grad, f_weight, g_weight, gains):
    channels = out_pair.shape[1] // 2
    pair_now = out_pair
    grad_now = out_grad
    pairs, grads, first_sums, second_sums, gain_sums = ([], [], [], [], [])
    for layer_index in range(N_SECTION - 1, -1, -1):
        results = coupling_back(pair_now[:, :channels], pair_now[:, channels:], grad_now[:, :channels].astype(jnp.float32), grad_now[:, channels:].astype(jnp.float32), f_weight[layer_index], g_weight[layer_index], gains[layer_index])
        pair_now = jnp.concatenate([results[0], results[1]], axis=1)
        grad_now = jnp.concatenate([results[2], results[3]], axis=1)
        pairs.append(pair_now)
        grads.append(grad_now)
        first_sums.append(replica_sum(results[4], results[5]))
        second_sums.append(replica_sum(results[6], results[7]))
        gain_sums.append(results[8])
    return (jnp.stack(pairs[::-1]), jnp.stack(grads[::-1]), jnp.stack(first_sums[::-1]), jnp.stack(second_sums[::-1]), jnp.stack(gain_sums[::-1]))
```

```python
import functools

import jax
import jax.numpy as jnp
from jax import lax
from jax.experimental import pallas as pl
from jax.experimental.pallas import tpu as pltpu
from jax.sharding import PartitionSpec as P

offset = 0.25
MESH = pl.DeviceIdType.MESH
f32, bf16 = jnp.float32, jnp.bfloat16


def silu_parts(pre_values):
    sigmoid_value = jax.nn.sigmoid(pre_values)
    return (pre_values * sigmoid_value, sigmoid_value * (1.0 + pre_values * (1.0 - sigmoid_value)))


def inverse_scale(values):
    return lax.rsqrt(jnp.mean(values * values, axis=-1, keepdims=True) + offset)


def kernel(
    n, sections, blocks,
    pair_ref, grad_ref, fw_ref, gw_ref, gains_ref,
    in_pair_ref, in_grad_ref, f_out, g_out, gain_out,
    wf, wg, wft, wgt, relay, rx, tx, held, slopes, norms_own, norms, deltas, result_tx, result_rx, gain_acc, gain_parts,
    go_sem, w_send, w_recv, r_send, r_recv, feed_send,
    p_send, p_recv, m_send, m_recv, n_send, n_recv, d_send, d_recv, c_send, c_recv, e_send, e_recv,
):
    s, d = lax.axis_index("section"), lax.axis_index("dp")
    m = n // 2
    half = sections // 2
    tokens = pair_ref.shape[0]
    h = pair_ref.shape[1] // 2
    part = fw_ref.shape[0]
    rows_all = 2 * tokens
    rows_per = rows_all // blocks
    own_blocks = blocks // 2

    pair_index = lax.div(d, 2)
    parity = lax.rem(pair_index, 2)
    host, mate = 2 * pair_index + 1 - parity, 2 * pair_index + parity
    is_host, is_mate = d == host, d == mate
    hosts = [2 * j + 1 - j % 2 for j in range(m)]

    is_last = s == sections - 1
    has_below = s > 0
    not_last = jnp.logical_not(is_last)
    partner = lax.rem(s + half, sections)
    high, low = s >= half, s < half
    both = jnp.logical_and

    chained = half % 2 == 0
    odd = lax.rem(s, 2) == 1
    even = jnp.logical_not(odd)
    crossing = jnp.where(high, s - half + 1, s + half - 1)
    crosses = both(even, high) | both(odd, low)
    follows = jnp.logical_not(both(odd, high))
    leads = jnp.logical_not(both(even, low))
    follower = jnp.where(odd, s - 1, crossing)
    feeds = both(s == half, is_mate)
    is_fed = both(is_last, is_host)

    barrier = pltpu.get_barrier_semaphore()

    def greet(section, replica):
        pl.semaphore_signal(barrier, inc=1, device_id=(section, replica), device_id_type=MESH)

    for k in range(1, n):
        greet(s, lax.rem(d + k, n))
    for k in range(n):
        greet(partner, lax.rem(d + k, n))

    @pl.when(has_below)
    def _():
        greet(s - 1, d)

    @pl.when(not_last)
    def _():
        greet(s + 1, d)

    @pl.when(feeds)
    def _():
        greet(sections - 1, host)

    @pl.when(is_fed)
    def _():
        greet(half, mate)

    neighbours = 2 * n - 1 + has_below.astype(jnp.int32) + not_last.astype(jnp.int32)
    neighbours += feeds.astype(jnp.int32) + is_fed.astype(jnp.int32)
    if chained:
        @pl.when(crosses)
        def _():
            greet(crossing, d)

        neighbours += crosses.astype(jnp.int32)
    pl.semaphore_wait(barrier, neighbours)

    fulls, owns = (wf, wg), (fw_ref, gw_ref)
    order = (1, 0)
    pieces = 2
    first, second = pl.ds(0, h), pl.ds(h, h)

    def wait_bytes(ref, sem):
        pltpu.make_async_copy(ref, ref, sem).wait()

    def send(src, dst, send_sem, recv_sem, section, replica):
        pltpu.make_async_remote_copy(
            src_ref=src, dst_ref=dst, send_sem=send_sem, recv_sem=recv_sem,
            device_id=(section, replica), device_id_type=MESH,
        ).start()

    def shard(a, owner, lead=0, size=part):
        start = pl.multiple_of(owner * part, part) + lead
        return fulls[a].at[pl.ds(pl.multiple_of(start, size), size)]

    def block_rows(b):
        return pl.ds(pl.multiple_of(b * rows_per, rows_per), rows_per)

    @pl.when(feeds)
    def _():
        for i, (source, column) in enumerate(
            ((pair_ref, first), (pair_ref, second), (grad_ref, first), (grad_ref, second))
        ):
            tx[i, pl.ds(tokens, tokens)] = source[:, column].astype(bf16)
        for b in range(own_blocks, blocks):
            for i in (0, 1, 3, 2):
                rows = block_rows(b)
                send(
                    tx.at[i, rows], rx.at[i, rows], feed_send, p_recv.at[i, b],
                    sections - 1, host,
                )

    def weights_out():
        if chained:
            @pl.when(follows)
            def _():
                pl.semaphore_wait(go_sem, 1)

        @pl.when(is_host)
        def _():
            for a in order:
                for t in hosts:
                    @pl.when(d != t)
                    def _():
                        send(owns[a], shard(a, d), w_send.at[a], w_recv.at[a], s, t)
            for a in order:
                fulls[a][pl.ds(pl.multiple_of(d * part, part), part), :] = owns[a][...]
            if m > 1:
                for a in order:
                    wait_bytes(fulls[a].at[pl.ds(0, (m - 1) * part)], w_send.at[a])

        @pl.when(is_mate)
        def _():
            for a in order:
                if m > 1:
                    for c in range(pieces):
                        size = part // pieces
                        rows = pl.ds(c * size, size)
                        send(
                            owns[a].at[rows], relay.at[a, rows], w_send.at[a], r_recv.at[a, c],
                            partner, d,
                        )
                send(owns[a], shard(a, d), w_send.at[a], w_recv.at[a], s, host)
            for a in order:
                wait_bytes(fulls[a].at[pl.ds(0, (2 if m > 1 else 1) * part)], w_send.at[a])

        if chained:
            @pl.when(leads)
            def _():
                pl.semaphore_signal(go_sem, inc=1, device_id=(follower, d), device_id_type=MESH)

    def pass_on():
        if m > 1:
            for a in order:
                for c in range(pieces):
                    size = part // pieces
                    rows = pl.ds(c * size, size)
                    wait_bytes(relay.at[a, rows], r_recv.at[a, c])
                    for t in hosts:
                        @pl.when(host != t)
                        def _():
                            send(
                                relay.at[a, rows], shard(a, d, c * size, size), r_send,
                                w_recv.at[a], partner, t,
                            )

    @pl.when(both(is_mate, low))
    def _():
        pass_on()

    weights_out()

    @pl.when(both(is_mate, high))
    def _():
        pass_on()

    def take(i, b, rows, source, column):
        local = both(is_last, b < own_blocks)

        @pl.when(local)
        def _():
            held[i] = source[rows, column].astype(f32)

        @pl.when(jnp.logical_not(local))
        def _():
            wait_bytes(rx.at[i, rows], p_recv.at[i, b])
            held[i] = rx[i, rows].astype(f32)

    def give(i, b, rows, values):
        tx[i, rows] = values.astype(bf16)

        @pl.when(has_below)
        def _():
            send(tx.at[i, rows], rx.at[i, rows], p_send, p_recv.at[i, b], s - 1, d)

        @pl.when(b >= own_blocks)
        def _():
            send(tx.at[i, rows], rx.at[i, rows], m_send, m_recv.at[i, b], s, mate)

    def share_norm(a, rows):
        for j, t in enumerate(hosts):
            @pl.when(d != t)
            def _():
                send(
                    norms_own.at[a, pl.ds(2 * j, 2), rows],
                    norms.at[a, pl.ds(0, 2), pair_index, rows],
                    n_send.at[a], n_recv.at[a], s, t,
                )

    def share_delta(a, rows):
        for t in hosts:
            @pl.when(d != t)
            def _():
                send(
                    deltas.at[a, pair_index, rows], deltas.at[a, pair_index, rows],
                    d_send.at[a], d_recv.at[a], s, t,
                )

    def block(b, carry):
        rows = block_rows(b)
        is_own = b < own_blocks
        gain_f, gain_g = gains_ref[0:1, :], gains_ref[1:2, :]
        take(0, b, rows, pair_ref, first)
        y1 = held[0]
        r1 = inverse_scale(y1)
        norm_g = (y1 * r1 * gain_g).astype(bf16)
        pre_g = jnp.dot(norm_g, wg[...], preferred_element_type=f32)
        take(1, b, rows, pair_ref, second)
        act_g, slope_g = silu_parts(pre_g)
        x2 = held[1] - act_g
        give(1, b, rows, x2)
        held[1] = x2
        slopes[0] = slope_g

        @pl.when(is_own)
        def _():
            in_pair_ref[rows, second] = x2

        r2 = inverse_scale(x2)
        norm_f = (x2 * r2 * gain_f).astype(bf16)

        @pl.when(b == 0)
        def _():
            wait_bytes(wf.at[pl.ds(0, (n - 1) * part)], w_recv.at[0])

        pre_f = jnp.dot(norm_f, wf[...], preferred_element_type=f32)
        act_f, slope_f = silu_parts(pre_f)
        x1 = held[0] - act_f
        give(0, b, rows, x1)
        slopes[1] = slope_f

        @pl.when(is_own)
        def _():
            in_pair_ref[rows, first] = x1

        for e in range(n):
            norms_own[0, e, rows] = norm_f[:, e * part:(e + 1) * part]
            norms_own[1, e, rows] = norm_g[:, e * part:(e + 1) * part]

        @pl.when(low)
        def _():
            share_norm(1, rows)
            share_norm(0, rows)

        @pl.when(b == 0)
        def _():
            wgt[...] = wg[...].T
            wft[...] = wf[...].T

        take(3, b, rows, grad_ref, second)
        take(2, b, rows, grad_ref, first)
        delta_g = (held[3] * slopes[0]).astype(bf16)
        back_g = jnp.dot(delta_g, wgt[...], preferred_element_type=f32)
        deltas[1, pair_index, rows] = delta_g

        @pl.when(low)
        def _():
            share_delta(1, rows)

        y1 = held[0]
        weighted = gain_g * back_g
        gz = held[2] + r1 * weighted - y1 * (r1 * r1 * r1) * jnp.mean(
            weighted * y1, axis=-1, keepdims=True
        )
        give(2, b, rows, gz)

        @pl.when(is_own)
        def _():
            in_grad_ref[rows, first] = gz.astype(bf16)

        gain_acc[1:2, :] += jnp.sum(back_g * y1 * r1, axis=0, keepdims=True)
        delta_f = (gz * slopes[1]).astype(bf16)
        back_f = jnp.dot(delta_f, wft[...], preferred_element_type=f32)
        deltas[0, pair_index, rows] = delta_f

        @pl.when(low)
        def _():
            share_delta(0, rows)

        x2 = held[1]
        weighted = gain_f * back_f
        gx2 = held[3] + r2 * weighted - x2 * (r2 * r2 * r2) * jnp.mean(
            weighted * x2, axis=-1, keepdims=True
        )
        give(3, b, rows, gx2)

        @pl.when(is_own)
        def _():
            in_grad_ref[rows, second] = gx2.astype(bf16)

        gain_acc[0:1, :] += jnp.sum(back_f * x2 * r2, axis=0, keepdims=True)
        return carry

    whole = pl.ds(0, rows_all)
    outs = (f_out, g_out)

    def product(a, which):
        return lax.dot_general(
            norms[a, which].reshape(m * rows_all, part), deltas[a].reshape(m * rows_all, h),
            (((0,), (0,)), ((), ())), preferred_element_type=f32,
        )

    @pl.when(is_host)
    def _():
        gain_acc[...] = jnp.zeros_like(gain_acc)
        wait_bytes(wg.at[pl.ds(0, (n - 1) * part)], w_recv.at[1])
        lax.fori_loop(0, blocks, block, 0)

        @pl.when(high)
        def _():
            for a in order:
                share_norm(a, whole)
                share_delta(a, whole)

        gain_parts[pair_index] = gain_acc[...]
        for k in range(1, n):
            send(
                gain_parts.at[pair_index], gain_parts.at[pair_index], c_send, c_recv,
                s, lax.rem(d + k, n),
            )
        for a in range(2):
            for w in range(2):
                norms[a, w, pair_index] = norms_own[a, 2 * pair_index + w]
        for a in order:
            if m > 1:
                wait_bytes(norms.at[a, pl.ds(0, 2), pl.ds(0, m - 1)], n_recv.at[a])
                wait_bytes(deltas.at[a, pl.ds(0, m - 1)], d_recv.at[a])
            result_tx[a] = product(a, parity).astype(bf16)
            send(result_tx.at[a], result_rx.at[a], e_send.at[a], e_recv.at[a], s, mate)
        for a in order:
            outs[a][...] = product(a, 1 - parity)

    @pl.when(is_mate)
    def _():
        def collect(b, carry):
            rows = block_rows(b + own_blocks)
            local = block_rows(b)
            for i, target, column in (
                (1, in_pair_ref, second), (0, in_pair_ref, first),
                (2, in_grad_ref, first), (3, in_grad_ref, second),
            ):
                wait_bytes(rx.at[i, rows], m_recv.at[i, b + own_blocks])
                target[local, column] = rx[i, rows].astype(target.dtype)
            return carry

        lax.fori_loop(0, own_blocks, collect, 0)
        for a in order:
            wait_bytes(result_rx.at[a], e_recv.at[a])
            outs[a][...] = result_rx[a].astype(f32)

    @pl.when(is_mate)
    def _():
        wait_bytes(gain_parts.at[pl.ds(0, m)], c_recv)

    if m > 1:
        @pl.when(is_host)
        def _():
            wait_bytes(gain_parts.at[pl.ds(0, m - 1)], c_recv)

    total = gain_parts[0]
    for j in range(1, m):
        total = total + gain_parts[j]
    gain_out[...] = total

    @pl.when(is_host)
    def _():
        wait_bytes(gain_parts.at[pl.ds(0, n - 1)], c_send)
        for a in range(2):
            wait_bytes(result_tx.at[a], e_send.at[a])
            if m > 1:
                wait_bytes(norms.at[a, pl.ds(0, 2), pl.ds(0, m - 1)], n_send.at[a])
                wait_bytes(deltas.at[a, pl.ds(0, m - 1)], d_send.at[a])
        wait_bytes(tx.at[:, pl.ds(0, tokens)], m_send)

        @pl.when(has_below)
        def _():
            wait_bytes(tx, p_send)

    if m > 1:
        @pl.when(is_mate)
        def _():
            for k in range(m - 1):
                wait_bytes(relay, r_send)

    @pl.when(feeds)
    def _():
        wait_bytes(tx.at[:, pl.ds(0, tokens)], feed_send)


def shards(out_pair, out_grad, f_weight, g_weight, gains):
    n, sections = lax.axis_size("dp"), lax.axis_size("section")
    tokens, width = out_pair.shape
    h = width // 2
    part = f_weight.shape[1]
    blocks = 4
    m = n // 2
    rows_all = 2 * tokens
    vmem = pl.BlockSpec(memory_space=pltpu.VMEM)
    dma = pltpu.SemaphoreType.DMA
    outs = pl.pallas_call(
        functools.partial(kernel, n, sections, blocks),
        out_shape=(
            jax.ShapeDtypeStruct((tokens, width), f32),
            jax.ShapeDtypeStruct((tokens, width), bf16),
            jax.ShapeDtypeStruct((part, h), f32),
            jax.ShapeDtypeStruct((part, h), f32),
            jax.ShapeDtypeStruct((2, h), f32),
        ),
        in_specs=[vmem] * 5,
        out_specs=[vmem] * 5,
        scratch_shapes=[
            pltpu.VMEM((h, h), bf16),
            pltpu.VMEM((h, h), bf16),
            pltpu.VMEM((h, h), bf16),
            pltpu.VMEM((h, h), bf16),
            pltpu.VMEM((2, part, h), bf16),
            pltpu.VMEM((4, rows_all, h), bf16),
            pltpu.VMEM((4, rows_all, h), bf16),
            pltpu.VMEM((4, rows_all // blocks, h), f32),
            pltpu.VMEM((2, rows_all // blocks, h), f32),
            pltpu.VMEM((2, n, rows_all, part), bf16),
            pltpu.VMEM((2, 2, m, rows_all, part), bf16),
            pltpu.VMEM((2, m, rows_all, h), bf16),
            pltpu.VMEM((2, part, h), bf16),
            pltpu.VMEM((2, part, h), bf16),
            pltpu.VMEM((2, h), f32),
            pltpu.VMEM((n, 2, h), f32),
            pltpu.SemaphoreType.REGULAR,
            dma((2,)),
            dma((2,)),
            dma,
            dma((2, 2)),
            dma,
            dma,
            dma((4, blocks)),
            dma,
            dma((4, blocks)),
            dma((2,)),
            dma((2,)),
            dma((2,)),
            dma((2,)),
            dma,
            dma,
            dma((2,)),
            dma((2,)),
        ],
        compiler_params=pltpu.CompilerParams(
            collective_id=0, has_side_effects=True, vmem_limit_bytes=60 * 1024 * 1024
        ),
    )(out_pair, out_grad, f_weight[0], g_weight[0], gains[0])
    return tuple(out[None] for out in outs)


def solution(mesh):
    placed = (
        P("dp", None),
        P("dp", None),
        P("section", "dp", None),
        P("section", "dp", None),
        P("section", None, None),
    )
    return jax.shard_map(
        shards,
        mesh=mesh,
        in_specs=placed,
        out_specs=(
            P("section", "dp", None),
            P("section", "dp", None),
            P("section", "dp", None),
            P("section", "dp", None),
            P("section", None, None),
        ),
        check_vma=False,
    )
```

```python
import functools

import jax
import jax.numpy as jnp
from jax import lax
from jax.experimental import pallas as pl
from jax.experimental.pallas import tpu as pltpu
from jax.sharding import PartitionSpec as P

offset = 0.25
MESH = pl.DeviceIdType.MESH
f32, bf16 = jnp.float32, jnp.bfloat16


def silu_parts(pre_values):
    sigmoid_value = jax.nn.sigmoid(pre_values)
    return (pre_values * sigmoid_value, sigmoid_value * (1.0 + pre_values * (1.0 - sigmoid_value)))


def inverse_scale(values):
    return lax.rsqrt(jnp.mean(values * values, axis=-1, keepdims=True) + offset)


def kernel(
    n, sections, blocks,
    pair_ref, grad_ref, fw_ref, gw_ref, gains_ref,
    in_pair_ref, in_grad_ref, f_out, g_out, gain_out,
    wf, wg, wft, wgt, relay, rx, tx, held, slopes, norms_own, norms, deltas, result_tx, result_rx, gain_acc, gain_parts,
    go_sem, clear_sem, w_send, w_recv, r_send, r_recv, feed_send,
    p_send, p_recv, m_send, m_recv, n_send, n_recv, d_send, d_recv, c_send, c_recv, e_send, e_recv,
):
    s, d = lax.axis_index("section"), lax.axis_index("dp")
    m = n // 2
    half = sections // 2
    tokens = pair_ref.shape[0]
    h = pair_ref.shape[1] // 2
    part = fw_ref.shape[0]
    rows_all = 2 * tokens
    rows_per = rows_all // blocks
    own_blocks = blocks // 2

    pair_index = lax.div(d, 2)
    parity = lax.rem(pair_index, 2)
    host, mate = 2 * pair_index + 1 - parity, 2 * pair_index + parity
    is_host, is_mate = d == host, d == mate
    hosts = [2 * j + 1 - j % 2 for j in range(m)]

    is_last = s == sections - 1
    has_below = s > 0
    not_last = jnp.logical_not(is_last)
    partner = lax.rem(s + half, sections)
    high, low = s >= half, s < half
    both = jnp.logical_and

    chained = half % 2 == 0
    odd = lax.rem(s, 2) == 1
    even = jnp.logical_not(odd)
    follows = jnp.logical_not(both(odd, high))
    splits = both(even, high)
    halves = both(even, low)
    holds = both(both(odd, low), s > 1)
    early = both(splits, s < sections - 2)
    feeder = max(sections - 3, 0)
    feeds = both(s == feeder, is_mate)
    is_fed = both(is_last, is_host)

    barrier = pltpu.get_barrier_semaphore()

    def greet(section, replica):
        pl.semaphore_signal(barrier, inc=1, device_id=(section, replica), device_id_type=MESH)

    for k in range(1, n):
        greet(s, lax.rem(d + k, n))
    for k in range(n):
        greet(partner, lax.rem(d + k, n))

    @pl.when(has_below)
    def _():
        greet(s - 1, d)

    @pl.when(not_last)
    def _():
        greet(s + 1, d)

    @pl.when(feeds)
    def _():
        greet(sections - 1, host)

    @pl.when(is_fed)
    def _():
        greet(feeder, mate)

    neighbours = 2 * n - 1 + has_below.astype(jnp.int32) + not_last.astype(jnp.int32)
    neighbours += feeds.astype(jnp.int32) + is_fed.astype(jnp.int32)
    if chained:
        @pl.when(splits)
        def _():
            greet(s - half + 1, d)

        @pl.when(both(odd, low))
        def _():
            greet(s + half - 1, d)

        neighbours += (splits | both(odd, low)).astype(jnp.int32)

        @pl.when(both(high, both(even, is_mate)))
        def _():
            greet(s + 1, host)

        @pl.when(both(high, both(odd, is_host)))
        def _():
            greet(s - 1, mate)

        neighbours += both(high, both(even, is_mate) | both(odd, is_host)).astype(jnp.int32)
    pl.semaphore_wait(barrier, neighbours)

    fulls, owns = (wf, wg), (fw_ref, gw_ref)
    order = (1, 0)
    pieces = 4
    first, second = pl.ds(0, h), pl.ds(h, h)

    def wait_bytes(ref, sem):
        pltpu.make_async_copy(ref, ref, sem).wait()

    def send(src, dst, send_sem, recv_sem, section, replica):
        pltpu.make_async_remote_copy(
            src_ref=src, dst_ref=dst, send_sem=send_sem, recv_sem=recv_sem,
            device_id=(section, replica), device_id_type=MESH,
        ).start()

    def shard(a, owner, lead=0, size=part):
        start = pl.multiple_of(owner * part, part) + lead
        return fulls[a].at[pl.ds(pl.multiple_of(start, size), size)]

    def block_rows(b):
        return pl.ds(pl.multiple_of(b * rows_per, rows_per), rows_per)

    def place_of(b):
        later = jnp.where(b <= own_blocks, b - 1 + own_blocks, b - own_blocks)
        return jnp.where(b == 0, 0, later)

    def feed():
        for i, (source, column) in enumerate(
            ((pair_ref, first), (pair_ref, second), (grad_ref, first), (grad_ref, second))
        ):
            tx[i, pl.ds(tokens, tokens)] = source[:, column].astype(bf16)
        for b in range(own_blocks, blocks):
            for i in (0, 1, 3, 2):
                rows = block_rows(b)
                send(
                    tx.at[i, rows], rx.at[i, rows], feed_send, p_recv.at[i, b],
                    sections - 1, host,
                )

    def go_low():
        go(s - half + 1)

    def go(section):
        pl.semaphore_signal(go_sem, inc=1, device_id=(section, d), device_id_type=MESH)

    def sent(a):
        if chained:
            @pl.when(early if a == order[0] else both(splits, jnp.logical_not(early)))
            def _():
                go_low()

            if a == order[1]:
                @pl.when(odd)
                def _():
                    go(s - 1)

    def weights_out():
        if chained:
            @pl.when(follows)
            def _():
                pl.semaphore_wait(go_sem, 1)

        @pl.when(is_host)
        def _():
            for a in order:
                for t in hosts:
                    @pl.when(d != t)
                    def _():
                        send(owns[a], shard(a, d), w_send.at[a], w_recv.at[a], s, t)
            for a in order:
                fulls[a][pl.ds(pl.multiple_of(d * part, part), part), :] = owns[a][...]
            for a in order:
                if m > 1:
                    wait_bytes(fulls[a].at[pl.ds(0, (m - 1) * part)], w_send.at[a])
                sent(a)

        @pl.when(is_mate)
        def _():
            for a in order:
                if m > 1:
                    size = part // pieces
                    for c in range(pieces):
                        rows = pl.ds(c * size, size)
                        relayed = True if c < pieces // 2 else jnp.logical_not(halves)

                        @pl.when(relayed)
                        def _():
                            send(
                                owns[a].at[rows], relay.at[a, rows], w_send.at[a],
                                r_recv.at[a, c], partner, d,
                            )
                send(owns[a], shard(a, d), w_send.at[a], w_recv.at[a], s, host)
                if m > 1:
                    @pl.when(halves)
                    def _():
                        lead = part // 2
                        for t in hosts:
                            @pl.when(host != t)
                            def _():
                                send(
                                    owns[a].at[pl.ds(lead, lead)], shard(a, d, lead, lead),
                                    w_send.at[a], w_recv.at[a], s, t,
                                )
            for a in order:
                if m > 1:
                    @pl.when(halves)
                    def _():
                        lead = part // 2
                        wait_bytes(fulls[a].at[pl.ds(0, part + m * lead)], w_send.at[a])

                    @pl.when(jnp.logical_not(halves))
                    def _():
                        wait_bytes(fulls[a].at[pl.ds(0, 2 * part)], w_send.at[a])
                else:
                    wait_bytes(fulls[a].at[pl.ds(0, part)], w_send.at[a])
                sent(a)

    def pass_on():
        if m > 1:
            size = part // pieces
            for a in order:
                for c in range(pieces):
                    rows = pl.ds(c * size, size)
                    relayed = True if c < pieces // 2 else jnp.logical_not(splits)

                    @pl.when(relayed)
                    def _():
                        wait_bytes(relay.at[a, rows], r_recv.at[a, c])
                        for t in hosts:
                            @pl.when(host != t)
                            def _():
                                send(
                                    relay.at[a, rows], shard(a, d, c * size, size), r_send,
                                    w_recv.at[a], partner, t,
                                )

    def passed_on():
        if m > 1:
            @pl.when(splits)
            def _():
                for k in range(m - 1):
                    wait_bytes(relay.at[0], r_send)

            @pl.when(jnp.logical_not(splits))
            def _():
                for k in range(m - 1):
                    wait_bytes(relay, r_send)

    def clear(section):
        pl.semaphore_signal(clear_sem, inc=1, device_id=(section, host), device_id_type=MESH)

    @pl.when(both(is_mate, low))
    def _():
        pass_on()

    weights_out()

    @pl.when(feeds)
    def _():
        feed()

    @pl.when(both(is_mate, high))
    def _():
        pass_on()
        passed_on()

        if chained:
            @pl.when(even)
            def _():
                clear(s)
                clear(s + 1)
        else:
            clear(s)

    def take(i, b, rows, source, column):
        local = both(is_last, b < own_blocks)

        @pl.when(local)
        def _():
            held[i] = source[rows, column].astype(f32)

        @pl.when(jnp.logical_not(local))
        def _():
            wait_bytes(rx.at[i, rows], p_recv.at[i, b])
            held[i] = rx[i, rows].astype(f32)

    def give(i, b, rows, values):
        tx[i, rows] = values.astype(bf16)

        @pl.when(has_below)
        def _():
            send(tx.at[i, rows], rx.at[i, rows], p_send, p_recv.at[i, b], s - 1, d)

        @pl.when(b >= own_blocks)
        def _():
            send(tx.at[i, rows], rx.at[i, rows], m_send, m_recv.at[i, b], s, mate)

    def share_norm(a, rows):
        for j, t in enumerate(hosts):
            @pl.when(d != t)
            def _():
                send(
                    norms_own.at[a, pl.ds(2 * j, 2), rows],
                    norms.at[a, pl.ds(0, 2), pair_index, rows],
                    n_send.at[a], n_recv.at[a], s, t,
                )

    def share_delta(a, rows):
        for t in hosts:
            @pl.when(d != t)
            def _():
                send(
                    deltas.at[a, pair_index, rows], deltas.at[a, pair_index, rows],
                    d_send.at[a], d_recv.at[a], s, t,
                )

    def block(step, carry):
        b = place_of(step)
        rows = block_rows(b)
        is_own = b < own_blocks
        gain_f, gain_g = gains_ref[0:1, :], gains_ref[1:2, :]
        take(0, b, rows, pair_ref, first)
        y1 = held[0]
        r1 = inverse_scale(y1)
        norm_g = (y1 * r1 * gain_g).astype(bf16)
        pre_g = jnp.dot(norm_g, wg[...], preferred_element_type=f32)
        take(1, b, rows, pair_ref, second)
        act_g, slope_g = silu_parts(pre_g)
        x2 = held[1] - act_g
        give(1, b, rows, x2)
        held[1] = x2
        slopes[0] = slope_g

        @pl.when(is_own)
        def _():
            in_pair_ref[rows, second] = x2

        r2 = inverse_scale(x2)
        norm_f = (x2 * r2 * gain_f).astype(bf16)

        @pl.when(step == 0)
        def _():
            wait_bytes(wf.at[pl.ds(0, (n - 1) * part)], w_recv.at[0])

        pre_f = jnp.dot(norm_f, wf[...], preferred_element_type=f32)
        act_f, slope_f = silu_parts(pre_f)
        x1 = held[0] - act_f
        give(0, b, rows, x1)
        slopes[1] = slope_f

        @pl.when(is_own)
        def _():
            in_pair_ref[rows, first] = x1

        for e in range(n):
            norms_own[0, e, rows] = norm_f[:, e * part:(e + 1) * part]
            norms_own[1, e, rows] = norm_g[:, e * part:(e + 1) * part]

        streams = both(low, jnp.logical_not(both(holds, step < blocks // 2)))

        @pl.when(streams)
        def _():
            share_norm(1, rows)
            share_norm(0, rows)

        @pl.when(step == 0)
        def _():
            wgt[...] = wg[...].T
            wft[...] = wf[...].T

        take(3, b, rows, grad_ref, second)
        take(2, b, rows, grad_ref, first)
        delta_g = (held[3] * slopes[0]).astype(bf16)
        back_g = jnp.dot(delta_g, wgt[...], preferred_element_type=f32)
        deltas[1, pair_index, rows] = delta_g

        @pl.when(streams)
        def _():
            share_delta(1, rows)

        y1 = held[0]
        weighted = gain_g * back_g
        gz = held[2] + r1 * weighted - y1 * (r1 * r1 * r1) * jnp.mean(
            weighted * y1, axis=-1, keepdims=True
        )
        give(2, b, rows, gz)

        @pl.when(is_own)
        def _():
            in_grad_ref[rows, first] = gz.astype(bf16)

        gain_acc[1:2, :] += jnp.sum(back_g * y1 * r1, axis=0, keepdims=True)
        delta_f = (gz * slopes[1]).astype(bf16)
        back_f = jnp.dot(delta_f, wft[...], preferred_element_type=f32)
        deltas[0, pair_index, rows] = delta_f

        x2 = held[1]
        weighted = gain_f * back_f
        gx2 = held[3] + r2 * weighted - x2 * (r2 * r2 * r2) * jnp.mean(
            weighted * x2, axis=-1, keepdims=True
        )
        give(3, b, rows, gx2)

        @pl.when(is_own)
        def _():
            in_grad_ref[rows, second] = gx2.astype(bf16)

        gain_acc[0:1, :] += jnp.sum(back_f * x2 * r2, axis=0, keepdims=True)
        return carry

    whole = pl.ds(0, rows_all)
    outs = (f_out, g_out)

    def product(a, which):
        return lax.dot_general(
            norms[a, which].reshape(m * rows_all, part), deltas[a].reshape(m * rows_all, h),
            (((0,), (0,)), ((), ())), preferred_element_type=f32,
        )

    @pl.when(is_host)
    def _():
        gain_acc[...] = jnp.zeros_like(gain_acc)
        wait_bytes(wg.at[pl.ds(0, (n - 1) * part)], w_recv.at[1])
        lax.fori_loop(0, blocks, block, 0)

        @pl.when(high)
        def _():
            pl.semaphore_wait(clear_sem, 1)
            for a in order:
                share_norm(a, whole)
                share_delta(a, whole)

        @pl.when(holds)
        def _():
            for step in range(blocks // 2):
                place = 0 if step == 0 else step - 1 + own_blocks
                rows = pl.ds(place * rows_per, rows_per)
                share_norm(1, rows)
                share_delta(1, rows)
                share_norm(0, rows)

        @pl.when(low)
        def _():
            share_delta(0, whole)

        gain_parts[pair_index] = gain_acc[...]
        for k in range(1, n):
            send(
                gain_parts.at[pair_index], gain_parts.at[pair_index], c_send, c_recv,
                s, lax.rem(d + k, n),
            )
        for a in range(2):
            for w in range(2):
                norms[a, w, pair_index] = norms_own[a, 2 * pair_index + w]
        for a in order:
            if m > 1:
                wait_bytes(norms.at[a, pl.ds(0, 2), pl.ds(0, m - 1)], n_recv.at[a])
                wait_bytes(deltas.at[a, pl.ds(0, m - 1)], d_recv.at[a])
            result_tx[a] = product(a, parity).astype(bf16)
            send(result_tx.at[a], result_rx.at[a], e_send.at[a], e_recv.at[a], s, mate)
        for a in order:
            outs[a][...] = product(a, 1 - parity)

    @pl.when(is_mate)
    def _():
        def collect(b, carry):
            rows = block_rows(b + own_blocks)
            local = block_rows(b)
            for i, target, column in (
                (1, in_pair_ref, second), (0, in_pair_ref, first),
                (2, in_grad_ref, first), (3, in_grad_ref, second),
            ):
                wait_bytes(rx.at[i, rows], m_recv.at[i, b + own_blocks])
                target[local, column] = rx[i, rows].astype(target.dtype)
            return carry

        lax.fori_loop(0, own_blocks, collect, 0)
        for a in order:
            wait_bytes(result_rx.at[a], e_recv.at[a])
            outs[a][...] = result_rx[a].astype(f32)

    @pl.when(is_mate)
    def _():
        wait_bytes(gain_parts.at[pl.ds(0, m)], c_recv)

    if m > 1:
        @pl.when(is_host)
        def _():
            wait_bytes(gain_parts.at[pl.ds(0, m - 1)], c_recv)

    total = gain_parts[0]
    for j in range(1, m):
        total = total + gain_parts[j]
    gain_out[...] = total

    @pl.when(is_host)
    def _():
        wait_bytes(gain_parts.at[pl.ds(0, n - 1)], c_send)
        for a in range(2):
            wait_bytes(result_tx.at[a], e_send.at[a])
            if m > 1:
                wait_bytes(norms.at[a, pl.ds(0, 2), pl.ds(0, m - 1)], n_send.at[a])
                wait_bytes(deltas.at[a, pl.ds(0, m - 1)], d_send.at[a])
        wait_bytes(tx.at[:, pl.ds(0, tokens)], m_send)

        @pl.when(has_below)
        def _():
            wait_bytes(tx, p_send)

    @pl.when(both(is_mate, low))
    def _():
        passed_on()

    @pl.when(feeds)
    def _():
        wait_bytes(tx.at[:, pl.ds(0, tokens)], feed_send)


def shards(out_pair, out_grad, f_weight, g_weight, gains):
    n, sections = lax.axis_size("dp"), lax.axis_size("section")
    tokens, width = out_pair.shape
    h = width // 2
    part = f_weight.shape[1]
    blocks = 8
    m = n // 2
    rows_all = 2 * tokens
    vmem = pl.BlockSpec(memory_space=pltpu.VMEM)
    dma = pltpu.SemaphoreType.DMA
    outs = pl.pallas_call(
        functools.partial(kernel, n, sections, blocks),
        out_shape=(
            jax.ShapeDtypeStruct((tokens, width), f32),
            jax.ShapeDtypeStruct((tokens, width), bf16),
            jax.ShapeDtypeStruct((part, h), f32),
            jax.ShapeDtypeStruct((part, h), f32),
            jax.ShapeDtypeStruct((2, h), f32),
        ),
        in_specs=[vmem] * 5,
        out_specs=[vmem] * 5,
        scratch_shapes=[
            pltpu.VMEM((h, h), bf16),
            pltpu.VMEM((h, h), bf16),
            pltpu.VMEM((h, h), bf16),
            pltpu.VMEM((h, h), bf16),
            pltpu.VMEM((2, part, h), bf16),
            pltpu.VMEM((4, rows_all, h), bf16),
            pltpu.VMEM((4, rows_all, h), bf16),
            pltpu.VMEM((4, rows_all // blocks, h), f32),
            pltpu.VMEM((2, rows_all // blocks, h), f32),
            pltpu.VMEM((2, n, rows_all, part), bf16),
            pltpu.VMEM((2, 2, m, rows_all, part), bf16),
            pltpu.VMEM((2, m, rows_all, h), bf16),
            pltpu.VMEM((2, part, h), bf16),
            pltpu.VMEM((2, part, h), bf16),
            pltpu.VMEM((2, h), f32),
            pltpu.VMEM((n, 2, h), f32),
            pltpu.SemaphoreType.REGULAR,
            pltpu.SemaphoreType.REGULAR,
            dma((2,)),
            dma((2,)),
            dma,
            dma((2, 4)),
            dma,
            dma,
            dma((4, blocks)),
            dma,
            dma((4, blocks)),
            dma((2,)),
            dma((2,)),
            dma((2,)),
            dma((2,)),
            dma,
            dma,
            dma((2,)),
            dma((2,)),
        ],
        compiler_params=pltpu.CompilerParams(
            collective_id=0, has_side_effects=True, vmem_limit_bytes=60 * 1024 * 1024
        ),
    )(out_pair, out_grad, f_weight[0], g_weight[0], gains[0])
    return tuple(out[None] for out in outs)


def solution(mesh):
    placed = (
        P("dp", None),
        P("dp", None),
        P("section", "dp", None),
        P("section", "dp", None),
        P("section", None, None),
    )
    return jax.shard_map(
        shards,
        mesh=mesh,
        in_specs=placed,
        out_specs=(
            P("section", "dp", None),
            P("section", "dp", None),
            P("section", "dp", None),
            P("section", "dp", None),
            P("section", None, None),
        ),
        check_vma=False,
    )
```

```python
import functools

import jax
import jax.numpy as jnp
from jax import lax
from jax.experimental import pallas as pl
from jax.experimental.pallas import tpu as pltpu
from jax.sharding import PartitionSpec as P

offset = 0.25
MESH = pl.DeviceIdType.MESH
f32, bf16 = jnp.float32, jnp.bfloat16


def silu_parts(pre_values):
    sigmoid_value = jax.nn.sigmoid(pre_values)
    return (pre_values * sigmoid_value, sigmoid_value * (1.0 + pre_values * (1.0 - sigmoid_value)))


def inverse_scale(values):
    return lax.rsqrt(jnp.mean(values * values, axis=-1, keepdims=True) + offset)


def kernel(
    n, sections, blocks,
    pair_ref, grad_ref, fw_ref, gw_ref, gains_ref,
    in_pair_ref, in_grad_ref, f_out, g_out, gain_out,
    wf, wg, wft, wgt, relay, rx, tx, held, slopes, norms_own, norms, deltas, result_tx, result_rx, gain_acc, gain_parts, via, delta_via,
    go_sem, clear_sem, w_send, w_recv, r_send, r_recv, feed_send,
    p_send, p_recv, m_send, m_recv, n_send, n_recv, d_send, d_recv, c_send, c_recv, e_send, e_recv, v_send, v_recv, y_send, y_recv,
):
    s, d = lax.axis_index("section"), lax.axis_index("dp")
    m = n // 2
    half = sections // 2
    tokens = pair_ref.shape[0]
    h = pair_ref.shape[1] // 2
    part = fw_ref.shape[0]
    rows_all = 2 * tokens
    rows_per = rows_all // blocks
    own_blocks = blocks // 2

    pair_index = lax.div(d, 2)
    parity = lax.rem(pair_index, 2)
    host, mate = 2 * pair_index + 1 - parity, 2 * pair_index + parity
    is_host, is_mate = d == host, d == mate
    hosts = [2 * j + 1 - j % 2 for j in range(m)]

    is_last = s == sections - 1
    has_below = s > 0
    not_last = jnp.logical_not(is_last)
    partner = lax.rem(s + half, sections)
    high, low = s >= half, s < half
    both = jnp.logical_and

    chained = half % 2 == 0
    odd = lax.rem(s, 2) == 1
    even = jnp.logical_not(odd)
    follows = jnp.logical_not(both(odd, high))
    splits = both(even, high)
    halves = both(even, low)
    early = both(splits, s < sections - 2)
    waits = both(high, s >= sections - 2) if chained else high
    holds = jnp.logical_not(waits) & (high | both(odd, s > 1))
    routed = s < 2
    routes = both(high, s - half < 2)
    feeder = max(sections - 3, 0)
    feeds = both(s == feeder, is_mate)
    is_fed = both(is_last, is_host)

    barrier = pltpu.get_barrier_semaphore()

    def greet(section, replica):
        pl.semaphore_signal(barrier, inc=1, device_id=(section, replica), device_id_type=MESH)

    for k in range(1, n):
        greet(s, lax.rem(d + k, n))
    for k in range(n):
        greet(partner, lax.rem(d + k, n))

    @pl.when(has_below)
    def _():
        greet(s - 1, d)

    @pl.when(not_last)
    def _():
        greet(s + 1, d)

    @pl.when(feeds)
    def _():
        greet(sections - 1, host)

    @pl.when(is_fed)
    def _():
        greet(feeder, mate)

    neighbours = 2 * n - 1 + has_below.astype(jnp.int32) + not_last.astype(jnp.int32)
    neighbours += feeds.astype(jnp.int32) + is_fed.astype(jnp.int32)
    if chained:
        @pl.when(splits)
        def _():
            greet(s - half + 1, d)

        @pl.when(both(odd, low))
        def _():
            greet(s + half - 1, d)

        neighbours += (splits | both(odd, low)).astype(jnp.int32)

        @pl.when(both(high, both(even, is_mate)))
        def _():
            greet(s + 1, host)

        @pl.when(both(high, both(odd, is_host)))
        def _():
            greet(s - 1, mate)

        neighbours += both(high, both(even, is_mate) | both(odd, is_host)).astype(jnp.int32)
    pl.semaphore_wait(barrier, neighbours)

    fulls, owns = (wf, wg), (fw_ref, gw_ref)
    order = (1, 0)
    pieces = 4
    first, second = pl.ds(0, h), pl.ds(h, h)
    every = pl.ds(0, h)

    def wait_bytes(ref, sem):
        pltpu.make_async_copy(ref, ref, sem).wait()

    def send(src, dst, send_sem, recv_sem, section, replica):
        pltpu.make_async_remote_copy(
            src_ref=src, dst_ref=dst, send_sem=send_sem, recv_sem=recv_sem,
            device_id=(section, replica), device_id_type=MESH,
        ).start()

    def shard(a, owner, lead=0, size=part):
        start = pl.multiple_of(owner * part, part) + lead
        return fulls[a].at[pl.ds(pl.multiple_of(start, size), size)]

    def block_rows(b):
        return pl.ds(pl.multiple_of(b * rows_per, rows_per), rows_per)

    def place_of(b):
        later = jnp.where(b <= own_blocks, b - 1 + own_blocks, b - own_blocks)
        return jnp.where(b == 0, 0, later)

    def feed():
        for i, (source, column) in enumerate(
            ((pair_ref, first), (pair_ref, second), (grad_ref, first), (grad_ref, second))
        ):
            tx[i, pl.ds(tokens, tokens)] = source[:, column].astype(bf16)
        for b in range(own_blocks, blocks):
            for i in (0, 1, 3, 2):
                rows = block_rows(b)
                send(
                    tx.at[i, rows], rx.at[i, rows], feed_send, p_recv.at[i, b],
                    sections - 1, host,
                )

    def go_low():
        go(s - half + 1)

    def go(section):
        pl.semaphore_signal(go_sem, inc=1, device_id=(section, d), device_id_type=MESH)

    def sent(a):
        if chained:
            @pl.when(early if a == order[0] else both(splits, jnp.logical_not(early)))
            def _():
                go_low()

            if a == order[1]:
                @pl.when(odd)
                def _():
                    go(s - 1)

    def weights_out():
        if chained:
            @pl.when(follows)
            def _():
                pl.semaphore_wait(go_sem, 1)

        @pl.when(is_host)
        def _():
            for a in order:
                for t in hosts:
                    @pl.when(d != t)
                    def _():
                        send(owns[a], shard(a, d), w_send.at[a], w_recv.at[a], s, t)
            for a in order:
                fulls[a][pl.ds(pl.multiple_of(d * part, part), part), :] = owns[a][...]
            for a in order:
                if m > 1:
                    wait_bytes(fulls[a].at[pl.ds(0, (m - 1) * part)], w_send.at[a])
                sent(a)

        @pl.when(is_mate)
        def _():
            for a in order:
                if m > 1:
                    size = part // pieces
                    for c in range(pieces):
                        rows = pl.ds(c * size, size)
                        relayed = True if c < pieces // 2 else jnp.logical_not(halves)

                        @pl.when(relayed)
                        def _():
                            send(
                                owns[a].at[rows], relay.at[a, rows], w_send.at[a],
                                r_recv.at[a, c], partner, d,
                            )
                send(owns[a], shard(a, d), w_send.at[a], w_recv.at[a], s, host)
                if m > 1:
                    @pl.when(halves)
                    def _():
                        lead = part // 2
                        for t in hosts:
                            @pl.when(host != t)
                            def _():
                                send(
                                    owns[a].at[pl.ds(lead, lead)], shard(a, d, lead, lead),
                                    w_send.at[a], w_recv.at[a], s, t,
                                )
            for a in order:
                if m > 1:
                    @pl.when(halves)
                    def _():
                        lead = part // 2
                        wait_bytes(fulls[a].at[pl.ds(0, part + m * lead)], w_send.at[a])

                    @pl.when(jnp.logical_not(halves))
                    def _():
                        wait_bytes(fulls[a].at[pl.ds(0, 2 * part)], w_send.at[a])
                else:
                    wait_bytes(fulls[a].at[pl.ds(0, part)], w_send.at[a])
                sent(a)

    def pass_on():
        if m > 1:
            size = part // pieces
            for a in order:
                for c in range(pieces):
                    rows = pl.ds(c * size, size)
                    relayed = True if c < pieces // 2 else jnp.logical_not(splits)

                    @pl.when(relayed)
                    def _():
                        wait_bytes(relay.at[a, rows], r_recv.at[a, c])
                        for t in hosts:
                            @pl.when(host != t)
                            def _():
                                send(
                                    relay.at[a, rows], shard(a, d, c * size, size), r_send,
                                    w_recv.at[a], partner, t,
                                )

    def passed_on():
        if m > 1:
            @pl.when(splits)
            def _():
                for k in range(m - 1):
                    wait_bytes(relay.at[0], r_send)

            @pl.when(jnp.logical_not(splits))
            def _():
                for k in range(m - 1):
                    wait_bytes(relay, r_send)

    def clear(section):
        pl.semaphore_signal(clear_sem, inc=1, device_id=(section, host), device_id_type=MESH)

    @pl.when(both(is_mate, low))
    def _():
        pass_on()

    weights_out()

    @pl.when(feeds)
    def _():
        feed()

    @pl.when(both(is_mate, high))
    def _():
        pass_on()
        passed_on()

        if chained:
            @pl.when(both(even, s >= sections - 2))
            def _():
                clear(s)
                clear(s + 1)
        else:
            clear(s)

    def take(i, b, rows, source, column):
        local = both(is_last, b < own_blocks)

        @pl.when(local)
        def _():
            held[i] = source[rows, column].astype(f32)

        @pl.when(jnp.logical_not(local))
        def _():
            wait_bytes(rx.at[i, rows], p_recv.at[i, b])
            held[i] = rx[i, rows].astype(f32)

    def give(i, b, rows, values):
        tx[i, rows] = values.astype(bf16)

        @pl.when(has_below)
        def _():
            send(tx.at[i, rows], rx.at[i, rows], p_send, p_recv.at[i, b], s - 1, d)

        @pl.when(b >= own_blocks)
        def _():
            send(tx.at[i, rows], rx.at[i, rows], m_send, m_recv.at[i, b], s, mate)

    def share_norm(a, rows):
        for j, t in enumerate(hosts):
            @pl.when(d != t)
            def _():
                send(
                    norms_own.at[a, pl.ds(2 * j, 2), rows],
                    norms.at[a, pl.ds(0, 2), pair_index, rows],
                    n_send.at[a], n_recv.at[a], s, t,
                )

    def share_delta(a, rows, cols, slot):
        for t in hosts:
            @pl.when(d != t)
            def _():
                send(
                    deltas.at[a, pair_index, rows, cols], deltas.at[a, pair_index, rows, cols],
                    d_send.at[slot], d_recv.at[slot], s, t,
                )

    left = pl.ds(0, via.shape[1])
    ways = ((1, every, 2), (0, left, 0), (0, pl.ds(left.size, h - left.size), 1))

    def route_delta(step, rows):
        send(
            deltas.at[0, pair_index, rows, left], delta_via.at[rows], d_send.at[0],
            y_recv.at[step], partner, host,
        )

    def forward(step, carry):
        rows = block_rows(place_of(step))
        wait_bytes(delta_via.at[rows], y_recv.at[step])
        for t in hosts:
            @pl.when(d != t)
            def _():
                send(
                    delta_via.at[rows], deltas.at[0, pair_index, rows, left],
                    y_send, d_recv.at[0], partner, t,
                )
        return carry

    def block(step, carry):
        b = place_of(step)
        rows = block_rows(b)
        is_own = b < own_blocks
        gain_f, gain_g = gains_ref[0:1, :], gains_ref[1:2, :]
        take(0, b, rows, pair_ref, first)
        y1 = held[0]
        r1 = inverse_scale(y1)
        norm_g = (y1 * r1 * gain_g).astype(bf16)
        pre_g = jnp.dot(norm_g, wg[...], preferred_element_type=f32)
        take(1, b, rows, pair_ref, second)
        act_g, slope_g = silu_parts(pre_g)
        x2 = held[1] - act_g
        give(1, b, rows, x2)
        held[1] = x2
        slopes[0] = slope_g

        @pl.when(is_own)
        def _():
            in_pair_ref[rows, second] = x2

        r2 = inverse_scale(x2)
        norm_f = (x2 * r2 * gain_f).astype(bf16)

        @pl.when(step == 0)
        def _():
            wait_bytes(wf.at[pl.ds(0, (n - 1) * part)], w_recv.at[0])

        pre_f = jnp.dot(norm_f, wf[...], preferred_element_type=f32)
        act_f, slope_f = silu_parts(pre_f)
        x1 = held[0] - act_f
        give(0, b, rows, x1)
        slopes[1] = slope_f

        @pl.when(is_own)
        def _():
            in_pair_ref[rows, first] = x1

        for e in range(n):
            norms_own[0, e, rows] = norm_f[:, e * part:(e + 1) * part]
            norms_own[1, e, rows] = norm_g[:, e * part:(e + 1) * part]

        streams = jnp.logical_not(waits | both(holds, step < blocks // 2))

        @pl.when(both(holds, step == blocks // 2))
        def _():
            for earlier in range(blocks // 2):
                place = 0 if earlier == 0 else earlier - 1 + own_blocks
                held_rows = pl.ds(place * rows_per, rows_per)
                share_norm(1, held_rows)
                share_delta(1, held_rows, every, 2)
                share_norm(0, held_rows)

        @pl.when(streams)
        def _():
            share_norm(1, rows)
            share_norm(0, rows)

        @pl.when(step == 0)
        def _():
            wgt[...] = wg[...].T
            wft[...] = wf[...].T

        take(3, b, rows, grad_ref, second)
        take(2, b, rows, grad_ref, first)
        delta_g = (held[3] * slopes[0]).astype(bf16)
        back_g = jnp.dot(delta_g, wgt[...], preferred_element_type=f32)
        deltas[1, pair_index, rows] = delta_g

        @pl.when(streams)
        def _():
            share_delta(1, rows, every, 2)

        y1 = held[0]
        weighted = gain_g * back_g
        gz = held[2] + r1 * weighted - y1 * (r1 * r1 * r1) * jnp.mean(
            weighted * y1, axis=-1, keepdims=True
        )
        give(2, b, rows, gz)

        @pl.when(is_own)
        def _():
            in_grad_ref[rows, first] = gz.astype(bf16)

        gain_acc[1:2, :] += jnp.sum(back_g * y1 * r1, axis=0, keepdims=True)
        delta_f = (gz * slopes[1]).astype(bf16)
        back_f = jnp.dot(delta_f, wft[...], preferred_element_type=f32)
        deltas[0, pair_index, rows] = delta_f

        @pl.when(routed)
        def _():
            route_delta(step, rows)

        x2 = held[1]
        weighted = gain_f * back_f
        gx2 = held[3] + r2 * weighted - x2 * (r2 * r2 * r2) * jnp.mean(
            weighted * x2, axis=-1, keepdims=True
        )
        give(3, b, rows, gx2)

        @pl.when(is_own)
        def _():
            in_grad_ref[rows, second] = gx2.astype(bf16)

        gain_acc[0:1, :] += jnp.sum(back_f * x2 * r2, axis=0, keepdims=True)
        return carry

    whole = pl.ds(0, rows_all)
    outs = (f_out, g_out)

    def product(a, which, cols):
        return lax.dot_general(
            norms[a, which].reshape(m * rows_all, part),
            deltas[a, :, :, cols].reshape(m * rows_all, cols.size),
            (((0,), (0,)), ((), ())), preferred_element_type=f32,
        )

    @pl.when(is_host)
    def _():
        gain_acc[...] = jnp.zeros_like(gain_acc)
        wait_bytes(wg.at[pl.ds(0, (n - 1) * part)], w_recv.at[1])
        lax.fori_loop(0, blocks, block, 0)

        @pl.when(waits)
        def _():
            pl.semaphore_wait(clear_sem, 1)
            share_norm(1, whole)
            share_delta(*ways[0][:1], whole, *ways[0][1:])
            share_norm(0, whole)
            for a, cols, slot in ways[1:]:
                share_delta(a, whole, cols, slot)

        @pl.when(jnp.logical_not(waits | routed))
        def _():
            share_delta(*ways[1][:1], whole, *ways[1][1:])

        @pl.when(jnp.logical_not(waits))
        def _():
            share_delta(*ways[2][:1], whole, *ways[2][1:])

        gain_parts[pair_index] = gain_acc[...]
        for k in range(1, n):
            send(
                gain_parts.at[pair_index], gain_parts.at[pair_index], c_send, c_recv,
                s, lax.rem(d + k, n),
            )
        for a in range(2):
            for w in range(2):
                norms[a, w, pair_index] = norms_own[a, 2 * pair_index + w]
        for a, cols, slot in ways:
            if m > 1:
                if slot != 1:
                    wait_bytes(norms.at[a, pl.ds(0, 2), pl.ds(0, m - 1)], n_recv.at[a])
                wait_bytes(deltas.at[a, pl.ds(0, m - 1), whole, cols], d_recv.at[slot])
            result_tx[a, :, cols] = product(a, parity, cols).astype(bf16)

            def direct():
                send(
                    result_tx.at[a, :, cols], result_rx.at[a, :, cols], e_send.at[slot],
                    e_recv.at[slot], s, mate,
                )

            if slot == 0:
                @pl.when(high)
                def _():
                    direct()

                @pl.when(low)
                def _():
                    for c in range(2):
                        lines = pl.ds(c * (part // 2), part // 2)
                        send(
                            result_tx.at[a, lines, cols], via.at[lines], e_send.at[slot],
                            v_recv.at[c], partner, host,
                        )
            else:
                direct()
        for a in order:
            outs[a][...] = product(a, 1 - parity, every)

        @pl.when(routes)
        def _():
            lax.fori_loop(0, blocks, forward, 0)

        @pl.when(high)
        def _():
            for c in range(2):
                lines = pl.ds(c * (part // 2), part // 2)
                wait_bytes(via.at[lines], v_recv.at[c])
                send(
                    via.at[lines], result_rx.at[0, lines, left], v_send, e_recv.at[0],
                    partner, mate,
                )

    @pl.when(is_mate)
    def _():
        def collect(b, carry):
            rows = block_rows(b + own_blocks)
            local = block_rows(b)
            for i, target, column in (
                (1, in_pair_ref, second), (0, in_pair_ref, first),
                (2, in_grad_ref, first), (3, in_grad_ref, second),
            ):
                wait_bytes(rx.at[i, rows], m_recv.at[i, b + own_blocks])
                target[local, column] = rx[i, rows].astype(target.dtype)
            return carry

        lax.fori_loop(0, own_blocks, collect, 0)
        for a, cols, slot in (ways[0], ways[2], ways[1]):
            wait_bytes(result_rx.at[a, :, cols], e_recv.at[slot])
            outs[a][:, cols] = result_rx[a, :, cols].astype(f32)

    @pl.when(is_mate)
    def _():
        wait_bytes(gain_parts.at[pl.ds(0, m)], c_recv)

    if m > 1:
        @pl.when(is_host)
        def _():
            wait_bytes(gain_parts.at[pl.ds(0, m - 1)], c_recv)

    total = gain_parts[0]
    for j in range(1, m):
        total = total + gain_parts[j]
    gain_out[...] = total

    @pl.when(is_host)
    def _():
        wait_bytes(gain_parts.at[pl.ds(0, n - 1)], c_send)
        for a, cols, slot in ways:
            wait_bytes(result_tx.at[a, :, cols], e_send.at[slot])
            if m > 1:
                if slot != 1:
                    wait_bytes(norms.at[a, pl.ds(0, 2), pl.ds(0, m - 1)], n_send.at[a])
                if slot == 0:
                    @pl.when(jnp.logical_not(routed))
                    def _():
                        wait_bytes(deltas.at[0, pl.ds(0, m - 1), whole, left], d_send.at[0])
                else:
                    wait_bytes(deltas.at[a, pl.ds(0, m - 1), whole, cols], d_send.at[slot])

        @pl.when(routed)
        def _():
            wait_bytes(delta_via, d_send.at[0])

        @pl.when(high)
        def _():
            wait_bytes(via, v_send)

        if m > 1:
            @pl.when(routes)
            def _():
                for k in range(m - 1):
                    wait_bytes(delta_via, y_send)

        wait_bytes(tx.at[:, pl.ds(0, tokens)], m_send)

        @pl.when(has_below)
        def _():
            wait_bytes(tx, p_send)

    @pl.when(both(is_mate, low))
    def _():
        passed_on()

    @pl.when(feeds)
    def _():
        wait_bytes(tx.at[:, pl.ds(0, tokens)], feed_send)


def put(*refs):
    k = len(refs) // 2
    sems = refs[-1]
    copies = [pltpu.make_async_copy(refs[i], refs[k + i], sems.at[i]) for i in range(k)]
    for copy in copies:
        copy.start()
    for copy in copies:
        copy.wait()


def shards(out_pair, out_grad, f_weight, g_weight, gains):
    n, sections = lax.axis_size("dp"), lax.axis_size("section")
    tokens, width = out_pair.shape
    h = width // 2
    part = f_weight.shape[1]
    blocks = 8
    m = n // 2
    rows_all = 2 * tokens
    split = h // 2
    vmem = pl.BlockSpec(memory_space=pltpu.VMEM)
    dma = pltpu.SemaphoreType.DMA
    outs = pl.pallas_call(
        functools.partial(kernel, n, sections, blocks),
        out_shape=(
            jax.ShapeDtypeStruct((tokens, width), f32),
            jax.ShapeDtypeStruct((tokens, width), bf16),
            jax.ShapeDtypeStruct((part, h), f32),
            jax.ShapeDtypeStruct((part, h), f32),
            jax.ShapeDtypeStruct((2, h), f32),
        ),
        in_specs=[vmem] * 5,
        out_specs=[vmem] * 5,
        scratch_shapes=[
            pltpu.VMEM((h, h), bf16),
            pltpu.VMEM((h, h), bf16),
            pltpu.VMEM((h, h), bf16),
            pltpu.VMEM((h, h), bf16),
            pltpu.VMEM((2, part, h), bf16),
            pltpu.VMEM((4, rows_all, h), bf16),
            pltpu.VMEM((4, rows_all, h), bf16),
            pltpu.VMEM((4, rows_all // blocks, h), f32),
            pltpu.VMEM((2, rows_all // blocks, h), f32),
            pltpu.VMEM((2, n, rows_all, part), bf16),
            pltpu.VMEM((2, 2, m, rows_all, part), bf16),
            pltpu.VMEM((2, m, rows_all, h), bf16),
            pltpu.VMEM((2, part, h), bf16),
            pltpu.VMEM((2, part, h), bf16),
            pltpu.VMEM((2, h), f32),
            pltpu.VMEM((n, 2, h), f32),
            pltpu.VMEM((part, split), bf16),
            pltpu.VMEM((rows_all, split), bf16),
            pltpu.SemaphoreType.REGULAR,
            pltpu.SemaphoreType.REGULAR,
            dma((2,)),
            dma((2,)),
            dma,
            dma((2, 4)),
            dma,
            dma,
            dma((4, blocks)),
            dma,
            dma((4, blocks)),
            dma((2,)),
            dma((2,)),
            dma((3,)),
            dma((3,)),
            dma,
            dma,
            dma((3,)),
            dma((3,)),
            dma,
            dma((2,)),
            dma,
            dma((blocks,)),
        ],
        compiler_params=pltpu.CompilerParams(
            collective_id=0, has_side_effects=True, vmem_limit_bytes=60 * 1024 * 1024
        ),
    )(out_pair, out_grad, f_weight[0], g_weight[0], gains[0])
    outs = pl.pallas_call(
        put,
        out_shape=tuple(jax.ShapeDtypeStruct(out.shape, out.dtype) for out in outs),
        in_specs=[vmem] * 5,
        out_specs=[pl.BlockSpec(memory_space=pl.ANY)] * 5,
        scratch_shapes=[dma((5,))],
        compiler_params=pltpu.CompilerParams(has_side_effects=False),
    )(*outs)
    return tuple(out[None] for out in outs)


def solution(mesh):
    placed = (
        P("dp", None),
        P("dp", None),
        P("section", "dp", None),
        P("section", "dp", None),
        P("section", None, None),
    )
    return jax.shard_map(
        shards,
        mesh=mesh,
        in_specs=placed,
        out_specs=(
            P("section", "dp", None),
            P("section", "dp", None),
            P("section", "dp", None),
            P("section", "dp", None),
            P("section", None, None),
        ),
        check_vma=False,
    )
```

```python
import functools

import jax
import jax.numpy as jnp
from jax import lax
from jax.experimental import pallas as pl
from jax.experimental.pallas import tpu as pltpu
from jax.sharding import PartitionSpec as P

offset = 0.25
MESH = pl.DeviceIdType.MESH
f32, bf16 = jnp.float32, jnp.bfloat16


def silu_parts(pre_values):
    sigmoid_value = jax.nn.sigmoid(pre_values)
    return (pre_values * sigmoid_value, sigmoid_value * (1.0 + pre_values * (1.0 - sigmoid_value)))


def inverse_scale(values):
    return lax.rsqrt(jnp.mean(values * values, axis=-1, keepdims=True) + offset)


def kernel(
    n, sections, blocks,
    pair_in, grad_in, fw_in, gw_in, gains_in,
    in_pair_out, in_grad_out, f_put, g_put, gain_out,
    pair_ref, grad_ref, fw_ref, gw_ref, gains_ref, in_pair_ref, in_grad_ref, f_out, g_out,
    wf, wg, wft, wgt, relay, rx, tx, held, slopes, norms_own, norms, deltas, result_tx, result_rx, gain_acc, gain_parts, via, delta_via, g_via,
    go_sem, clear_sem, w_send, w_recv, r_send, r_recv, feed_send,
    p_send, p_recv, m_send, m_recv, n_send, n_recv, d_send, d_recv, c_send, c_recv, e_send, e_recv, v_send, v_recv, y_send, y_recv, l_sem, o_sem,
):
    s, d = lax.axis_index("section"), lax.axis_index("dp")
    loads = [
        pltpu.make_async_copy(source, target, l_sem.at[i])
        for i, (source, target) in enumerate((
            (gw_in, gw_ref), (fw_in, fw_ref), (pair_in, pair_ref), (grad_in, grad_ref),
            (gains_in, gains_ref),
        ))
    ]
    for load in loads:
        load.start()
    puts = [
        pltpu.make_async_copy(source, target, o_sem.at[i])
        for i, (source, target) in enumerate((
            (f_out, f_put), (g_out, g_put), (in_pair_ref, in_pair_out), (in_grad_ref, in_grad_out),
        ))
    ]
    m = n // 2
    half = sections // 2
    tokens = pair_ref.shape[0]
    h = pair_ref.shape[1] // 2
    part = fw_ref.shape[0]
    rows_all = 2 * tokens
    rows_per = rows_all // blocks
    own_blocks = blocks // 2

    pair_index = lax.div(d, 2)
    parity = lax.rem(pair_index, 2)
    host, mate = 2 * pair_index + 1 - parity, 2 * pair_index + parity
    is_host, is_mate = d == host, d == mate
    hosts = [2 * j + 1 - j % 2 for j in range(m)]

    is_last = s == sections - 1
    has_below = s > 0
    not_last = jnp.logical_not(is_last)
    partner = lax.rem(s + half, sections)
    high, low = s >= half, s < half
    both = jnp.logical_and

    chained = half % 2 == 0
    odd = lax.rem(s, 2) == 1
    even = jnp.logical_not(odd)
    follows = jnp.logical_not(both(odd, high))
    splits = both(even, high)
    halves = both(even, low)
    early = both(splits, s < sections - 2)
    waits = both(high, s >= sections - 2) if chained else high
    holds = jnp.logical_not(waits) & (high | both(odd, s > 1))
    routed = s < 2
    routes = both(high, s - half < 2)
    feeder = max(sections - 3, 0)
    feeds = both(s == feeder, is_mate)
    is_fed = both(is_last, is_host)

    barrier = pltpu.get_barrier_semaphore()

    def greet(section, replica):
        pl.semaphore_signal(barrier, inc=1, device_id=(section, replica), device_id_type=MESH)

    for k in range(1, n):
        greet(s, lax.rem(d + k, n))
    for k in range(n):
        greet(partner, lax.rem(d + k, n))

    @pl.when(has_below)
    def _():
        greet(s - 1, d)

    @pl.when(not_last)
    def _():
        greet(s + 1, d)

    @pl.when(feeds)
    def _():
        greet(sections - 1, host)

    @pl.when(is_fed)
    def _():
        greet(feeder, mate)

    neighbours = 2 * n - 1 + has_below.astype(jnp.int32) + not_last.astype(jnp.int32)
    neighbours += feeds.astype(jnp.int32) + is_fed.astype(jnp.int32)
    if chained:
        @pl.when(splits)
        def _():
            greet(s - half + 1, d)

        @pl.when(both(odd, low))
        def _():
            greet(s + half - 1, d)

        neighbours += (splits | both(odd, low)).astype(jnp.int32)

        @pl.when(both(high, both(even, is_mate)))
        def _():
            greet(s + 1, host)

        @pl.when(both(high, both(odd, is_host)))
        def _():
            greet(s - 1, mate)

        neighbours += both(high, both(even, is_mate) | both(odd, is_host)).astype(jnp.int32)
    for load in loads:
        load.wait()
    pl.semaphore_wait(barrier, neighbours)

    fulls, owns = (wf, wg), (fw_ref, gw_ref)
    order = (1, 0)
    pieces = 4
    first, second = pl.ds(0, h), pl.ds(h, h)
    every = pl.ds(0, h)

    def wait_bytes(ref, sem):
        pltpu.make_async_copy(ref, ref, sem).wait()

    def send(src, dst, send_sem, recv_sem, section, replica):
        pltpu.make_async_remote_copy(
            src_ref=src, dst_ref=dst, send_sem=send_sem, recv_sem=recv_sem,
            device_id=(section, replica), device_id_type=MESH,
        ).start()

    def shard(a, owner, lead=0, size=part):
        start = pl.multiple_of(owner * part, part) + lead
        return fulls[a].at[pl.ds(pl.multiple_of(start, size), size)]

    def block_rows(b):
        return pl.ds(pl.multiple_of(b * rows_per, rows_per), rows_per)

    def place_of(b):
        later = jnp.where(b <= own_blocks, b - 1 + own_blocks, b - own_blocks)
        return jnp.where(b == 0, 0, later)

    def feed():
        for i, (source, column) in enumerate(
            ((pair_ref, first), (pair_ref, second), (grad_ref, first), (grad_ref, second))
        ):
            tx[i, pl.ds(tokens, tokens)] = source[:, column].astype(bf16)
        for b in range(own_blocks, blocks):
            for i in (0, 1, 3, 2):
                rows = block_rows(b)
                send(
                    tx.at[i, rows], rx.at[i, rows], feed_send, p_recv.at[i, b],
                    sections - 1, host,
                )

    def go_low():
        go(s - half + 1)

    def go(section):
        pl.semaphore_signal(go_sem, inc=1, device_id=(section, d), device_id_type=MESH)

    def sent(a):
        if chained:
            @pl.when(early if a == order[0] else both(splits, jnp.logical_not(early)))
            def _():
                go_low()

            if a == order[1]:
                @pl.when(odd)
                def _():
                    go(s - 1)

    def weights_out():
        if chained:
            @pl.when(follows)
            def _():
                pl.semaphore_wait(go_sem, 1)

        @pl.when(is_host)
        def _():
            for a in order:
                for t in hosts:
                    @pl.when(d != t)
                    def _():
                        send(owns[a], shard(a, d), w_send.at[a], w_recv.at[a], s, t)
            for a in order:
                fulls[a][pl.ds(pl.multiple_of(d * part, part), part), :] = owns[a][...]
            for a in order:
                if m > 1:
                    wait_bytes(fulls[a].at[pl.ds(0, (m - 1) * part)], w_send.at[a])
                sent(a)

        @pl.when(is_mate)
        def _():
            for a in order:
                if m > 1:
                    size = part // pieces
                    for c in range(pieces):
                        rows = pl.ds(c * size, size)
                        relayed = True if c < pieces // 2 else jnp.logical_not(halves)

                        @pl.when(relayed)
                        def _():
                            send(
                                owns[a].at[rows], relay.at[a, rows], w_send.at[a],
                                r_recv.at[a, c], partner, d,
                            )
                send(owns[a], shard(a, d), w_send.at[a], w_recv.at[a], s, host)
                if m > 1:
                    @pl.when(halves)
                    def _():
                        lead = part // 2
                        for t in hosts:
                            @pl.when(host != t)
                            def _():
                                send(
                                    owns[a].at[pl.ds(lead, lead)], shard(a, d, lead, lead),
                                    w_send.at[a], w_recv.at[a], s, t,
                                )
            for a in order:
                if m > 1:
                    @pl.when(halves)
                    def _():
                        lead = part // 2
                        wait_bytes(fulls[a].at[pl.ds(0, part + m * lead)], w_send.at[a])

                    @pl.when(jnp.logical_not(halves))
                    def _():
                        wait_bytes(fulls[a].at[pl.ds(0, 2 * part)], w_send.at[a])
                else:
                    wait_bytes(fulls[a].at[pl.ds(0, part)], w_send.at[a])
                sent(a)

    def pass_on():
        if m > 1:
            size = part // pieces
            for a in order:
                for c in range(pieces):
                    rows = pl.ds(c * size, size)
                    relayed = True if c < pieces // 2 else jnp.logical_not(splits)

                    @pl.when(relayed)
                    def _():
                        wait_bytes(relay.at[a, rows], r_recv.at[a, c])
                        for t in hosts:
                            @pl.when(host != t)
                            def _():
                                send(
                                    relay.at[a, rows], shard(a, d, c * size, size), r_send,
                                    w_recv.at[a], partner, t,
                                )

    def passed_on():
        if m > 1:
            @pl.when(splits)
            def _():
                for k in range(m - 1):
                    wait_bytes(relay.at[0], r_send)

            @pl.when(jnp.logical_not(splits))
            def _():
                for k in range(m - 1):
                    wait_bytes(relay, r_send)

    def clear(section):
        pl.semaphore_signal(clear_sem, inc=1, device_id=(section, host), device_id_type=MESH)

    @pl.when(both(is_mate, low))
    def _():
        pass_on()

    weights_out()

    @pl.when(feeds)
    def _():
        feed()

    @pl.when(both(is_mate, high))
    def _():
        pass_on()
        passed_on()

        if chained:
            @pl.when(both(even, s >= sections - 2))
            def _():
                clear(s)
                clear(s + 1)
        else:
            clear(s)

    def take(i, b, rows, source, column):
        local = both(is_last, b < own_blocks)

        @pl.when(local)
        def _():
            held[i] = source[rows, column].astype(f32)

        @pl.when(jnp.logical_not(local))
        def _():
            wait_bytes(rx.at[i, rows], p_recv.at[i, b])
            held[i] = rx[i, rows].astype(f32)

    def give(i, b, rows, values):
        tx[i, rows] = values.astype(bf16)

        @pl.when(has_below)
        def _():
            send(tx.at[i, rows], rx.at[i, rows], p_send, p_recv.at[i, b], s - 1, d)

        @pl.when(b >= own_blocks)
        def _():
            send(tx.at[i, rows], rx.at[i, rows], m_send, m_recv.at[i, b], s, mate)

    def share_norm(a, rows):
        for j, t in enumerate(hosts):
            @pl.when(d != t)
            def _():
                send(
                    norms_own.at[a, pl.ds(2 * j, 2), rows],
                    norms.at[a, pl.ds(0, 2), pair_index, rows],
                    n_send.at[a], n_recv.at[a], s, t,
                )

    def share_delta(a, rows, cols, slot):
        for t in hosts:
            @pl.when(d != t)
            def _():
                send(
                    deltas.at[a, pair_index, rows, cols], deltas.at[a, pair_index, rows, cols],
                    d_send.at[slot], d_recv.at[slot], s, t,
                )

    left = pl.ds(0, via.shape[1])
    ways = ((1, every, 2), (0, left, 0), (0, pl.ds(left.size, h - left.size), 1))

    def route_delta(step, rows):
        send(
            deltas.at[0, pair_index, rows, left], delta_via.at[rows], d_send.at[0],
            y_recv.at[step], partner, host,
        )

    def forward(step, carry):
        rows = block_rows(place_of(step))
        wait_bytes(delta_via.at[rows], y_recv.at[step])
        for t in hosts:
            @pl.when(d != t)
            def _():
                send(
                    delta_via.at[rows], deltas.at[0, pair_index, rows, left],
                    y_send, d_recv.at[0], partner, t,
                )
        return carry

    def block(step, carry):
        b = place_of(step)
        rows = block_rows(b)
        is_own = b < own_blocks
        gain_f, gain_g = gains_ref[0:1, :], gains_ref[1:2, :]
        take(0, b, rows, pair_ref, first)
        y1 = held[0]
        r1 = inverse_scale(y1)
        norm_g = (y1 * r1 * gain_g).astype(bf16)
        pre_g = jnp.dot(norm_g, wg[...], preferred_element_type=f32)
        take(1, b, rows, pair_ref, second)
        act_g, slope_g = silu_parts(pre_g)
        x2 = held[1] - act_g
        give(1, b, rows, x2)
        held[1] = x2
        slopes[0] = slope_g

        @pl.when(is_own)
        def _():
            in_pair_ref[rows, second] = x2

        r2 = inverse_scale(x2)
        norm_f = (x2 * r2 * gain_f).astype(bf16)

        @pl.when(step == 0)
        def _():
            wait_bytes(wf.at[pl.ds(0, (n - 1) * part)], w_recv.at[0])

        pre_f = jnp.dot(norm_f, wf[...], preferred_element_type=f32)
        act_f, slope_f = silu_parts(pre_f)
        x1 = held[0] - act_f
        give(0, b, rows, x1)
        slopes[1] = slope_f

        @pl.when(is_own)
        def _():
            in_pair_ref[rows, first] = x1

        for e in range(n):
            norms_own[0, e, rows] = norm_f[:, e * part:(e + 1) * part]
            norms_own[1, e, rows] = norm_g[:, e * part:(e + 1) * part]

        streams = jnp.logical_not(waits | both(holds, step < blocks // 2))

        @pl.when(both(holds, step == blocks // 2))
        def _():
            for earlier in range(blocks // 2):
                place = 0 if earlier == 0 else earlier - 1 + own_blocks
                held_rows = pl.ds(place * rows_per, rows_per)
                share_norm(1, held_rows)
                share_delta(1, held_rows, every, 2)
                share_norm(0, held_rows)

        @pl.when(streams)
        def _():
            share_norm(1, rows)
            share_norm(0, rows)

        @pl.when(step == 0)
        def _():
            wgt[...] = wg[...].T
            wft[...] = wf[...].T

        take(3, b, rows, grad_ref, second)
        take(2, b, rows, grad_ref, first)
        delta_g = (held[3] * slopes[0]).astype(bf16)
        back_g = jnp.dot(delta_g, wgt[...], preferred_element_type=f32)
        deltas[1, pair_index, rows] = delta_g

        @pl.when(streams)
        def _():
            share_delta(1, rows, every, 2)

        y1 = held[0]
        weighted = gain_g * back_g
        gz = held[2] + r1 * weighted - y1 * (r1 * r1 * r1) * jnp.mean(
            weighted * y1, axis=-1, keepdims=True
        )
        give(2, b, rows, gz)

        @pl.when(is_own)
        def _():
            in_grad_ref[rows, first] = gz.astype(bf16)

        gain_acc[1:2, :] += jnp.sum(back_g * y1 * r1, axis=0, keepdims=True)
        delta_f = (gz * slopes[1]).astype(bf16)
        back_f = jnp.dot(delta_f, wft[...], preferred_element_type=f32)
        deltas[0, pair_index, rows] = delta_f

        @pl.when(routed)
        def _():
            route_delta(step, rows)

        x2 = held[1]
        weighted = gain_f * back_f
        gx2 = held[3] + r2 * weighted - x2 * (r2 * r2 * r2) * jnp.mean(
            weighted * x2, axis=-1, keepdims=True
        )
        give(3, b, rows, gx2)

        @pl.when(is_own)
        def _():
            in_grad_ref[rows, second] = gx2.astype(bf16)

        gain_acc[0:1, :] += jnp.sum(back_f * x2 * r2, axis=0, keepdims=True)
        return carry

    whole = pl.ds(0, rows_all)
    outs = (f_out, g_out)

    def product(a, which, cols):
        return lax.dot_general(
            norms[a, which].reshape(m * rows_all, part),
            deltas[a, :, :, cols].reshape(m * rows_all, cols.size),
            (((0,), (0,)), ((), ())), preferred_element_type=f32,
        )

    @pl.when(is_host)
    def _():
        gain_acc[...] = jnp.zeros_like(gain_acc)
        wait_bytes(wg.at[pl.ds(0, (n - 1) * part)], w_recv.at[1])
        lax.fori_loop(0, blocks, block, 0)
        puts[2].start()
        puts[3].start()

        @pl.when(waits)
        def _():
            pl.semaphore_wait(clear_sem, 1)
            share_norm(1, whole)
            share_delta(*ways[0][:1], whole, *ways[0][1:])
            share_norm(0, whole)
            for a, cols, slot in ways[1:]:
                share_delta(a, whole, cols, slot)

        @pl.when(jnp.logical_not(waits | routed))
        def _():
            share_delta(*ways[1][:1], whole, *ways[1][1:])

        @pl.when(jnp.logical_not(waits))
        def _():
            share_delta(*ways[2][:1], whole, *ways[2][1:])

        gain_parts[pair_index] = gain_acc[...]
        for k in range(1, n):
            send(
                gain_parts.at[pair_index], gain_parts.at[pair_index], c_send, c_recv,
                s, lax.rem(d + k, n),
            )
        for a in range(2):
            for w in range(2):
                norms[a, w, pair_index] = norms_own[a, 2 * pair_index + w]
        for a, cols, slot in ways:
            if m > 1:
                if slot != 1:
                    wait_bytes(norms.at[a, pl.ds(0, 2), pl.ds(0, m - 1)], n_recv.at[a])
                wait_bytes(deltas.at[a, pl.ds(0, m - 1), whole, cols], d_recv.at[slot])
            result_tx[a, :, cols] = product(a, parity, cols).astype(bf16)

            def direct():
                send(
                    result_tx.at[a, :, cols], result_rx.at[a, :, cols], e_send.at[slot],
                    e_recv.at[slot], s, mate,
                )

            if slot == 2:
                head, end = pl.ds(0, part - g_via.shape[0]), pl.ds(part - g_via.shape[0], g_via.shape[0])
                send(
                    result_tx.at[1, head], result_rx.at[1, head], e_send.at[slot],
                    e_recv.at[slot], s, mate,
                )

                @pl.when(high)
                def _():
                    send(
                        result_tx.at[1, end], result_rx.at[1, end], e_send.at[slot],
                        e_recv.at[slot], s, mate,
                    )

                @pl.when(low)
                def _():
                    send(
                        result_tx.at[1, end], g_via, e_send.at[slot], v_recv.at[2],
                        partner, host,
                    )
            elif slot == 0:
                @pl.when(high)
                def _():
                    direct()

                @pl.when(low)
                def _():
                    for c in range(2):
                        lines = pl.ds(c * (part // 2), part // 2)
                        send(
                            result_tx.at[a, lines, cols], via.at[lines], e_send.at[slot],
                            v_recv.at[c], partner, host,
                        )
            else:
                direct()
        for a in order:
            outs[a][...] = product(a, 1 - parity, every)
            puts[a].start()

        @pl.when(routes)
        def _():
            lax.fori_loop(0, blocks, forward, 0)

        @pl.when(high)
        def _():
            wait_bytes(g_via, v_recv.at[2])
            end = pl.ds(part - g_via.shape[0], g_via.shape[0])
            send(g_via, result_rx.at[1, end], v_send.at[1], e_recv.at[2], partner, mate)
            for c in range(2):
                lines = pl.ds(c * (part // 2), part // 2)
                wait_bytes(via.at[lines], v_recv.at[c])
                send(
                    via.at[lines], result_rx.at[0, lines, left], v_send.at[0], e_recv.at[0],
                    partner, mate,
                )

    @pl.when(is_mate)
    def _():
        def collect(b, carry):
            rows = block_rows(b + own_blocks)
            local = block_rows(b)
            for i, target, column in (
                (1, in_pair_ref, second), (0, in_pair_ref, first),
                (2, in_grad_ref, first), (3, in_grad_ref, second),
            ):
                wait_bytes(rx.at[i, rows], m_recv.at[i, b + own_blocks])
                target[local, column] = rx[i, rows].astype(target.dtype)
            return carry

        lax.fori_loop(0, own_blocks, collect, 0)
        puts[2].start()
        puts[3].start()
        for a, cols, slot in (ways[0], ways[2], ways[1]):
            wait_bytes(result_rx.at[a, :, cols], e_recv.at[slot])
            outs[a][:, cols] = result_rx[a, :, cols].astype(f32)
            if slot != 1:
                puts[a].start()

    @pl.when(is_mate)
    def _():
        wait_bytes(gain_parts.at[pl.ds(0, m)], c_recv)

    if m > 1:
        @pl.when(is_host)
        def _():
            wait_bytes(gain_parts.at[pl.ds(0, m - 1)], c_recv)

    total = gain_parts[0]
    for j in range(1, m):
        total = total + gain_parts[j]
    gain_out[...] = total

    @pl.when(is_host)
    def _():
        wait_bytes(gain_parts.at[pl.ds(0, n - 1)], c_send)
        for a, cols, slot in ways:
            wait_bytes(result_tx.at[a, :, cols], e_send.at[slot])
            if m > 1:
                if slot != 1:
                    wait_bytes(norms.at[a, pl.ds(0, 2), pl.ds(0, m - 1)], n_send.at[a])
                if slot == 0:
                    @pl.when(jnp.logical_not(routed))
                    def _():
                        wait_bytes(deltas.at[0, pl.ds(0, m - 1), whole, left], d_send.at[0])
                else:
                    wait_bytes(deltas.at[a, pl.ds(0, m - 1), whole, cols], d_send.at[slot])

        @pl.when(routed)
        def _():
            wait_bytes(delta_via, d_send.at[0])

        @pl.when(high)
        def _():
            wait_bytes(via, v_send.at[0])
            wait_bytes(g_via, v_send.at[1])

        if m > 1:
            @pl.when(routes)
            def _():
                for k in range(m - 1):
                    wait_bytes(delta_via, y_send)

        wait_bytes(tx.at[:, pl.ds(0, tokens)], m_send)

        @pl.when(has_below)
        def _():
            wait_bytes(tx, p_send)

    @pl.when(both(is_mate, low))
    def _():
        passed_on()

    @pl.when(feeds)
    def _():
        wait_bytes(tx.at[:, pl.ds(0, tokens)], feed_send)

    for put in puts:
        put.wait()


def put(k, *refs):
    sources, targets, held = refs[:k], refs[k:2 * k], refs[2 * k:3 * k]
    in_sem, out_sem = refs[3 * k:]
    halves = []
    for i in range(k):
        rows = sources[i].shape[0]
        pieces = 2 if rows % 32 == 0 else 1
        for c in range(pieces):
            lines = pl.ds(c * (rows // pieces), rows // pieces)
            halves.append((
                pltpu.make_async_copy(
                    sources[i].at[lines], held[i].at[lines], in_sem.at[i, c]
                ),
                pltpu.make_async_copy(
                    held[i].at[lines], targets[i].at[lines], out_sem.at[i, c]
                ),
            ))
    for taken, _ in halves:
        taken.start()
    for taken, given in halves:
        taken.wait()
        given.start()
    for _, given in halves:
        given.wait()


def shards(out_pair, out_grad, f_weight, g_weight, gains):
    n, sections = lax.axis_size("dp"), lax.axis_size("section")
    tokens, width = out_pair.shape
    h = width // 2
    part = f_weight.shape[1]
    blocks = 8
    m = n // 2
    rows_all = 2 * tokens
    split = h // 2
    vmem, anywhere = pl.BlockSpec(memory_space=pltpu.VMEM), pl.BlockSpec(memory_space=pl.ANY)
    dma = pltpu.SemaphoreType.DMA
    outs = pl.pallas_call(
        functools.partial(kernel, n, sections, blocks),
        out_shape=(
            jax.ShapeDtypeStruct((tokens, width), f32),
            jax.ShapeDtypeStruct((tokens, width), bf16),
            jax.ShapeDtypeStruct((part, h), f32),
            jax.ShapeDtypeStruct((part, h), f32),
            jax.ShapeDtypeStruct((2, h), f32),
        ),
        in_specs=[anywhere] * 5,
        out_specs=[anywhere] * 4 + [vmem],
        scratch_shapes=[
            pltpu.VMEM((tokens, width), f32),
            pltpu.VMEM((tokens, width), bf16),
            pltpu.VMEM((part, h), bf16),
            pltpu.VMEM((part, h), bf16),
            pltpu.VMEM((2, h), f32),
            pltpu.VMEM((tokens, width), f32),
            pltpu.VMEM((tokens, width), bf16),
            pltpu.VMEM((part, h), f32),
            pltpu.VMEM((part, h), f32),
            pltpu.VMEM((h, h), bf16),
            pltpu.VMEM((h, h), bf16),
            pltpu.VMEM((h, h), bf16),
            pltpu.VMEM((h, h), bf16),
            pltpu.VMEM((2, part, h), bf16),
            pltpu.VMEM((4, rows_all, h), bf16),
            pltpu.VMEM((4, rows_all, h), bf16),
            pltpu.VMEM((4, rows_all // blocks, h), f32),
            pltpu.VMEM((2, rows_all // blocks, h), f32),
            pltpu.VMEM((2, n, rows_all, part), bf16),
            pltpu.VMEM((2, 2, m, rows_all, part), bf16),
            pltpu.VMEM((2, m, rows_all, h), bf16),
            pltpu.VMEM((2, part, h), bf16),
            pltpu.VMEM((2, part, h), bf16),
            pltpu.VMEM((2, h), f32),
            pltpu.VMEM((n, 2, h), f32),
            pltpu.VMEM((part, split), bf16),
            pltpu.VMEM((rows_all, split), bf16),
            pltpu.VMEM((part // 4, h), bf16),
            pltpu.SemaphoreType.REGULAR,
            pltpu.SemaphoreType.REGULAR,
            dma((2,)),
            dma((2,)),
            dma,
            dma((2, 4)),
            dma,
            dma,
            dma((4, blocks)),
            dma,
            dma((4, blocks)),
            dma((2,)),
            dma((2,)),
            dma((3,)),
            dma((3,)),
            dma,
            dma,
            dma((3,)),
            dma((3,)),
            dma((2,)),
            dma((3,)),
            dma,
            dma((blocks,)),
            dma((5,)),
            dma((4,)),
        ],
        compiler_params=pltpu.CompilerParams(
            collective_id=0, has_side_effects=True, vmem_limit_bytes=60 * 1024 * 1024
        ),
    )(out_pair, out_grad, f_weight[0], g_weight[0], gains[0])
    outs = pl.pallas_call(
        functools.partial(put, len(outs)),
        out_shape=tuple(jax.ShapeDtypeStruct(out.shape, out.dtype) for out in outs),
        in_specs=[anywhere] * len(outs),
        out_specs=[anywhere] * len(outs),
        scratch_shapes=[
            *(pltpu.VMEM(out.shape, out.dtype) for out in outs),
            dma((len(outs), 2)),
            dma((len(outs), 2)),
        ],
        compiler_params=pltpu.CompilerParams(vmem_limit_bytes=60 * 1024 * 1024),
    )(*outs)
    return tuple(out[None] for out in outs)


def solution(mesh):
    placed = (
        P("dp", None),
        P("dp", None),
        P("section", "dp", None),
        P("section", "dp", None),
        P("section", None, None),
    )
    return jax.shard_map(
        shards,
        mesh=mesh,
        in_specs=placed,
        out_specs=(
            P("section", "dp", None),
            P("section", "dp", None),
            P("section", "dp", None),
            P("section", "dp", None),
            P("section", None, None),
        ),
        check_vma=False,
    )
```

```python
import functools

import jax
import jax.numpy as jnp
from jax import lax
from jax.experimental import pallas as pl
from jax.experimental.pallas import tpu as pltpu
from jax.sharding import PartitionSpec as P

offset = 0.25
MESH = pl.DeviceIdType.MESH
f32, bf16 = jnp.float32, jnp.bfloat16


def silu_parts(pre_values):
    sigmoid_value = jax.nn.sigmoid(pre_values)
    return (pre_values * sigmoid_value, sigmoid_value * (1.0 + pre_values * (1.0 - sigmoid_value)))


def inverse_scale(values):
    return lax.rsqrt(jnp.mean(values * values, axis=-1, keepdims=True) + offset)


def kernel(
    n, sections, blocks,
    pair_in, grad_in, fw_in, gw_in, gains_in,
    in_pair_out, in_grad_out, f_put, g_put, gain_out,
    pair_ref, grad_ref, fw_ref, gw_ref, gains_ref, in_pair_ref, in_grad_ref, f_out, g_out,
    wf, wg, wft, wgt, relay, rx, tx, held, slopes, norms_own, norms, deltas, result_tx, result_rx, gain_acc, gain_parts, via, delta_via, g_via,
    go_sem, clear_sem, w_send, w_recv, r_send, r_recv, feed_send,
    p_send, p_recv, m_send, m_recv, n_send, n_recv, d_send, d_recv, c_send, c_recv, e_send, e_recv, v_send, v_recv, y_send, y_recv, l_sem, o_sem,
):
    s, d = lax.axis_index("section"), lax.axis_index("dp")
    loads = [
        pltpu.make_async_copy(source, target, l_sem.at[i])
        for i, (source, target) in enumerate((
            (gw_in, gw_ref), (fw_in, fw_ref), (pair_in, pair_ref), (grad_in, grad_ref),
            (gains_in, gains_ref),
        ))
    ]
    for load in loads:
        load.start()
    puts = [
        pltpu.make_async_copy(source, target, o_sem.at[i])
        for i, (source, target) in enumerate((
            (f_out, f_put), (g_out, g_put), (in_pair_ref, in_pair_out), (in_grad_ref, in_grad_out),
        ))
    ]
    split = via.shape[1]
    results = [
        pltpu.make_async_copy(result_rx.at[a, :, cols], target.at[:, cols], o_sem.at[slot])
        for a, target, cols, slot in (
            (0, f_put, pl.ds(0, split), 0),
            (1, g_put, pl.ds(0, g_put.shape[1]), 1),
            (0, f_put, pl.ds(split, f_put.shape[1] - split), 4),
        )
    ]
    m = n // 2
    half = sections // 2
    tokens = pair_ref.shape[0]
    h = pair_ref.shape[1] // 2
    part = fw_ref.shape[0]
    rows_all = 2 * tokens
    rows_per = rows_all // blocks
    own_blocks = blocks // 2

    pair_index = lax.div(d, 2)
    parity = lax.rem(pair_index, 2)
    host, mate = 2 * pair_index + 1 - parity, 2 * pair_index + parity
    is_host, is_mate = d == host, d == mate
    hosts = [2 * j + 1 - j % 2 for j in range(m)]

    is_last = s == sections - 1
    has_below = s > 0
    not_last = jnp.logical_not(is_last)
    partner = lax.rem(s + half, sections)
    high, low = s >= half, s < half
    both = jnp.logical_and

    chained = half % 2 == 0
    odd = lax.rem(s, 2) == 1
    even = jnp.logical_not(odd)
    follows = jnp.logical_not(both(odd, high))
    splits = both(even, high)
    halves = both(even, low)
    early = both(splits, s < sections - 2)
    waits = both(high, s >= sections - 2) if chained else high
    holds = jnp.logical_not(waits) & (high | both(odd, s > 1))
    routed = s < 2
    routes = both(high, s - half < 2)
    feeder = max(sections - 3, 0)
    feeds = both(s == feeder, is_mate)
    is_fed = both(is_last, is_host)

    barrier = pltpu.get_barrier_semaphore()

    def greet(section, replica):
        pl.semaphore_signal(barrier, inc=1, device_id=(section, replica), device_id_type=MESH)

    for k in range(1, n):
        greet(s, lax.rem(d + k, n))
    for k in range(n):
        greet(partner, lax.rem(d + k, n))

    @pl.when(has_below)
    def _():
        greet(s - 1, d)

    @pl.when(not_last)
    def _():
        greet(s + 1, d)

    @pl.when(feeds)
    def _():
        greet(sections - 1, host)

    @pl.when(is_fed)
    def _():
        greet(feeder, mate)

    neighbours = 2 * n - 1 + has_below.astype(jnp.int32) + not_last.astype(jnp.int32)
    neighbours += feeds.astype(jnp.int32) + is_fed.astype(jnp.int32)
    if chained:
        @pl.when(splits)
        def _():
            greet(s - half + 1, d)

        @pl.when(both(odd, low))
        def _():
            greet(s + half - 1, d)

        neighbours += (splits | both(odd, low)).astype(jnp.int32)

        @pl.when(both(high, both(even, is_mate)))
        def _():
            greet(s + 1, host)

        @pl.when(both(high, both(odd, is_host)))
        def _():
            greet(s - 1, mate)

        neighbours += both(high, both(even, is_mate) | both(odd, is_host)).astype(jnp.int32)
    for load in loads:
        load.wait()
    pl.semaphore_wait(barrier, neighbours)

    fulls, owns = (wf, wg), (fw_ref, gw_ref)
    order = (1, 0)
    pieces = 4
    first, second = pl.ds(0, h), pl.ds(h, h)
    every = pl.ds(0, h)

    def wait_bytes(ref, sem):
        pltpu.make_async_copy(ref, ref, sem).wait()

    def send(src, dst, send_sem, recv_sem, section, replica):
        pltpu.make_async_remote_copy(
            src_ref=src, dst_ref=dst, send_sem=send_sem, recv_sem=recv_sem,
            device_id=(section, replica), device_id_type=MESH,
        ).start()

    def shard(a, owner, lead=0, size=part):
        start = pl.multiple_of(owner * part, part) + lead
        return fulls[a].at[pl.ds(pl.multiple_of(start, size), size)]

    def block_rows(b):
        return pl.ds(pl.multiple_of(b * rows_per, rows_per), rows_per)

    def place_of(b):
        later = jnp.where(b <= own_blocks, b - 1 + own_blocks, b - own_blocks)
        return jnp.where(b == 0, 0, later)

    def feed():
        for i, (source, column) in enumerate(
            ((pair_ref, first), (pair_ref, second), (grad_ref, first), (grad_ref, second))
        ):
            tx[i, pl.ds(tokens, tokens)] = source[:, column].astype(bf16)
        for b in range(own_blocks, blocks):
            for i in (0, 1, 3, 2):
                rows = block_rows(b)
                send(
                    tx.at[i, rows], rx.at[i, rows], feed_send, p_recv.at[i, b],
                    sections - 1, host,
                )

    def go_low():
        go(s - half + 1)

    def go(section):
        pl.semaphore_signal(go_sem, inc=1, device_id=(section, d), device_id_type=MESH)

    def sent(a):
        if chained:
            @pl.when(early if a == order[0] else both(splits, jnp.logical_not(early)))
            def _():
                go_low()

            if a == order[1]:
                @pl.when(odd)
                def _():
                    go(s - 1)

    def weights_out():
        if chained:
            @pl.when(follows)
            def _():
                pl.semaphore_wait(go_sem, 1)

        @pl.when(is_host)
        def _():
            for a in order:
                for t in hosts:
                    @pl.when(d != t)
                    def _():
                        send(owns[a], shard(a, d), w_send.at[a], w_recv.at[a], s, t)
            for a in order:
                fulls[a][pl.ds(pl.multiple_of(d * part, part), part), :] = owns[a][...]
            for a in order:
                if m > 1:
                    wait_bytes(fulls[a].at[pl.ds(0, (m - 1) * part)], w_send.at[a])
                sent(a)

        @pl.when(is_mate)
        def _():
            for a in order:
                if m > 1:
                    size = part // pieces
                    for c in range(pieces):
                        rows = pl.ds(c * size, size)
                        relayed = True if c < pieces // 2 else jnp.logical_not(halves)

                        @pl.when(relayed)
                        def _():
                            send(
                                owns[a].at[rows], relay.at[a, rows], w_send.at[a],
                                r_recv.at[a, c], partner, d,
                            )
                send(owns[a], shard(a, d), w_send.at[a], w_recv.at[a], s, host)
                if m > 1:
                    @pl.when(halves)
                    def _():
                        lead = part // 2
                        for t in hosts:
                            @pl.when(host != t)
                            def _():
                                send(
                                    owns[a].at[pl.ds(lead, lead)], shard(a, d, lead, lead),
                                    w_send.at[a], w_recv.at[a], s, t,
                                )
            for a in order:
                if m > 1:
                    @pl.when(halves)
                    def _():
                        lead = part // 2
                        wait_bytes(fulls[a].at[pl.ds(0, part + m * lead)], w_send.at[a])

                    @pl.when(jnp.logical_not(halves))
                    def _():
                        wait_bytes(fulls[a].at[pl.ds(0, 2 * part)], w_send.at[a])
                else:
                    wait_bytes(fulls[a].at[pl.ds(0, part)], w_send.at[a])
                sent(a)

    def pass_on():
        if m > 1:
            size = part // pieces
            for a in order:
                for c in range(pieces):
                    rows = pl.ds(c * size, size)
                    relayed = True if c < pieces // 2 else jnp.logical_not(splits)

                    @pl.when(relayed)
                    def _():
                        wait_bytes(relay.at[a, rows], r_recv.at[a, c])
                        for t in hosts:
                            @pl.when(host != t)
                            def _():
                                send(
                                    relay.at[a, rows], shard(a, d, c * size, size), r_send,
                                    w_recv.at[a], partner, t,
                                )

    def passed_on():
        if m > 1:
            @pl.when(splits)
            def _():
                for k in range(m - 1):
                    wait_bytes(relay.at[0], r_send)

            @pl.when(jnp.logical_not(splits))
            def _():
                for k in range(m - 1):
                    wait_bytes(relay, r_send)

    def clear(section):
        pl.semaphore_signal(clear_sem, inc=1, device_id=(section, host), device_id_type=MESH)

    @pl.when(both(is_mate, low))
    def _():
        pass_on()

    weights_out()

    @pl.when(feeds)
    def _():
        feed()

    @pl.when(both(is_mate, high))
    def _():
        pass_on()
        passed_on()

        if chained:
            @pl.when(both(even, s >= sections - 2))
            def _():
                clear(s)
                clear(s + 1)
        else:
            clear(s)

    def take(i, b, rows, source, column):
        local = both(is_last, b < own_blocks)

        @pl.when(local)
        def _():
            held[i] = source[rows, column].astype(f32)

        @pl.when(jnp.logical_not(local))
        def _():
            wait_bytes(rx.at[i, rows], p_recv.at[i, b])
            held[i] = rx[i, rows].astype(f32)

    def give(i, b, rows, values):
        tx[i, rows] = values.astype(bf16)

        @pl.when(has_below)
        def _():
            send(tx.at[i, rows], rx.at[i, rows], p_send, p_recv.at[i, b], s - 1, d)

        @pl.when(b >= own_blocks)
        def _():
            send(tx.at[i, rows], rx.at[i, rows], m_send, m_recv.at[i, b], s, mate)

    def share_norm(a, rows):
        for j, t in enumerate(hosts):
            @pl.when(d != t)
            def _():
                send(
                    norms_own.at[a, pl.ds(2 * j, 2), rows],
                    norms.at[a, pl.ds(0, 2), pair_index, rows],
                    n_send.at[a], n_recv.at[a], s, t,
                )

    def share_delta(a, rows, cols, slot):
        for t in hosts:
            @pl.when(d != t)
            def _():
                send(
                    deltas.at[a, pair_index, rows, cols], deltas.at[a, pair_index, rows, cols],
                    d_send.at[slot], d_recv.at[slot], s, t,
                )

    left = pl.ds(0, via.shape[1])
    ways = ((1, every, 2), (0, left, 0), (0, pl.ds(left.size, h - left.size), 1))

    def route_delta(step, rows):
        send(
            deltas.at[0, pair_index, rows, left], delta_via.at[rows], d_send.at[0],
            y_recv.at[step], partner, host,
        )

    def forward(step, carry):
        rows = block_rows(place_of(step))
        wait_bytes(delta_via.at[rows], y_recv.at[step])
        for t in hosts:
            @pl.when(d != t)
            def _():
                send(
                    delta_via.at[rows], deltas.at[0, pair_index, rows, left],
                    y_send, d_recv.at[0], partner, t,
                )
        return carry

    def block(step, carry):
        b = place_of(step)
        rows = block_rows(b)
        is_own = b < own_blocks
        gain_f, gain_g = gains_ref[0:1, :], gains_ref[1:2, :]
        take(0, b, rows, pair_ref, first)
        y1 = held[0]
        r1 = inverse_scale(y1)
        norm_g = (y1 * r1 * gain_g).astype(bf16)
        pre_g = jnp.dot(norm_g, wg[...], preferred_element_type=f32)
        take(1, b, rows, pair_ref, second)
        act_g, slope_g = silu_parts(pre_g)
        x2 = held[1] - act_g
        give(1, b, rows, x2)
        held[1] = x2
        slopes[0] = slope_g

        @pl.when(is_own)
        def _():
            in_pair_ref[rows, second] = x2

        r2 = inverse_scale(x2)
        norm_f = (x2 * r2 * gain_f).astype(bf16)

        @pl.when(step == 0)
        def _():
            wait_bytes(wf.at[pl.ds(0, (n - 1) * part)], w_recv.at[0])

        pre_f = jnp.dot(norm_f, wf[...], preferred_element_type=f32)
        act_f, slope_f = silu_parts(pre_f)
        x1 = held[0] - act_f
        give(0, b, rows, x1)
        slopes[1] = slope_f

        @pl.when(is_own)
        def _():
            in_pair_ref[rows, first] = x1

        for e in range(n):
            norms_own[0, e, rows] = norm_f[:, e * part:(e + 1) * part]
            norms_own[1, e, rows] = norm_g[:, e * part:(e + 1) * part]

        streams = jnp.logical_not(waits | both(holds, step < blocks // 2))

        @pl.when(both(holds, step == blocks // 2))
        def _():
            for earlier in range(blocks // 2):
                place = 0 if earlier == 0 else earlier - 1 + own_blocks
                held_rows = pl.ds(place * rows_per, rows_per)
                share_norm(1, held_rows)
                share_delta(1, held_rows, every, 2)
                share_norm(0, held_rows)

        @pl.when(streams)
        def _():
            share_norm(1, rows)
            share_norm(0, rows)

        @pl.when(step == 0)
        def _():
            wgt[...] = wg[...].T
            wft[...] = wf[...].T

        take(3, b, rows, grad_ref, second)
        take(2, b, rows, grad_ref, first)
        delta_g = (held[3] * slopes[0]).astype(bf16)
        back_g = jnp.dot(delta_g, wgt[...], preferred_element_type=f32)
        deltas[1, pair_index, rows] = delta_g

        @pl.when(streams)
        def _():
            share_delta(1, rows, every, 2)

        y1 = held[0]
        weighted = gain_g * back_g
        gz = held[2] + r1 * weighted - y1 * (r1 * r1 * r1) * jnp.mean(
            weighted * y1, axis=-1, keepdims=True
        )
        give(2, b, rows, gz)

        @pl.when(is_own)
        def _():
            in_grad_ref[rows, first] = gz.astype(bf16)

        gain_acc[1:2, :] += jnp.sum(back_g * y1 * r1, axis=0, keepdims=True)
        delta_f = (gz * slopes[1]).astype(bf16)
        back_f = jnp.dot(delta_f, wft[...], preferred_element_type=f32)
        deltas[0, pair_index, rows] = delta_f

        @pl.when(routed)
        def _():
            route_delta(step, rows)

        x2 = held[1]
        weighted = gain_f * back_f
        gx2 = held[3] + r2 * weighted - x2 * (r2 * r2 * r2) * jnp.mean(
            weighted * x2, axis=-1, keepdims=True
        )
        give(3, b, rows, gx2)

        @pl.when(is_own)
        def _():
            in_grad_ref[rows, second] = gx2.astype(bf16)

        gain_acc[0:1, :] += jnp.sum(back_f * x2 * r2, axis=0, keepdims=True)
        return carry

    whole = pl.ds(0, rows_all)
    outs = (f_out, g_out)

    def product(a, which, cols):
        return lax.dot_general(
            norms[a, which].reshape(m * rows_all, part),
            deltas[a, :, :, cols].reshape(m * rows_all, cols.size),
            (((0,), (0,)), ((), ())), preferred_element_type=f32,
        )

    @pl.when(is_host)
    def _():
        gain_acc[...] = jnp.zeros_like(gain_acc)
        wait_bytes(wg.at[pl.ds(0, (n - 1) * part)], w_recv.at[1])
        lax.fori_loop(0, blocks, block, 0)
        puts[2].start()
        puts[3].start()

        @pl.when(waits)
        def _():
            pl.semaphore_wait(clear_sem, 1)
            share_norm(1, whole)
            share_delta(*ways[0][:1], whole, *ways[0][1:])
            share_norm(0, whole)
            for a, cols, slot in ways[1:]:
                share_delta(a, whole, cols, slot)

        @pl.when(jnp.logical_not(waits | routed))
        def _():
            share_delta(*ways[1][:1], whole, *ways[1][1:])

        @pl.when(jnp.logical_not(waits))
        def _():
            share_delta(*ways[2][:1], whole, *ways[2][1:])

        gain_parts[pair_index] = gain_acc[...]
        for k in range(1, n):
            send(
                gain_parts.at[pair_index], gain_parts.at[pair_index], c_send, c_recv,
                s, lax.rem(d + k, n),
            )
        for a in range(2):
            for w in range(2):
                norms[a, w, pair_index] = norms_own[a, 2 * pair_index + w]
        for a, cols, slot in ways:
            if m > 1:
                if slot != 1:
                    wait_bytes(norms.at[a, pl.ds(0, 2), pl.ds(0, m - 1)], n_recv.at[a])
                wait_bytes(deltas.at[a, pl.ds(0, m - 1), whole, cols], d_recv.at[slot])
            result_tx[a, :, cols] = product(a, parity, cols).astype(bf16)

            def direct():
                send(
                    result_tx.at[a, :, cols], result_rx.at[a, :, cols], e_send.at[slot],
                    e_recv.at[slot], s, mate,
                )

            if slot == 2:
                head, end = pl.ds(0, part - g_via.shape[0]), pl.ds(part - g_via.shape[0], g_via.shape[0])
                send(
                    result_tx.at[1, head], result_rx.at[1, head], e_send.at[slot],
                    e_recv.at[slot], s, mate,
                )

                @pl.when(high)
                def _():
                    send(
                        result_tx.at[1, end], result_rx.at[1, end], e_send.at[slot],
                        e_recv.at[slot], s, mate,
                    )

                @pl.when(low)
                def _():
                    send(
                        result_tx.at[1, end], g_via, e_send.at[slot], v_recv.at[2],
                        partner, host,
                    )
            elif slot == 0:
                @pl.when(high)
                def _():
                    direct()

                @pl.when(low)
                def _():
                    for c in range(2):
                        lines = pl.ds(c * (part // 2), part // 2)
                        send(
                            result_tx.at[a, lines, cols], via.at[lines], e_send.at[slot],
                            v_recv.at[c], partner, host,
                        )
            else:
                direct()
        for a in order:
            outs[a][...] = product(a, 1 - parity, every).astype(bf16)
            puts[a].start()

        @pl.when(routes)
        def _():
            lax.fori_loop(0, blocks, forward, 0)

        @pl.when(high)
        def _():
            wait_bytes(g_via, v_recv.at[2])
            end = pl.ds(part - g_via.shape[0], g_via.shape[0])
            send(g_via, result_rx.at[1, end], v_send.at[1], e_recv.at[2], partner, mate)
            for c in range(2):
                lines = pl.ds(c * (part // 2), part // 2)
                wait_bytes(via.at[lines], v_recv.at[c])
                send(
                    via.at[lines], result_rx.at[0, lines, left], v_send.at[0], e_recv.at[0],
                    partner, mate,
                )

    @pl.when(is_mate)
    def _():
        def collect(b, carry):
            rows = block_rows(b + own_blocks)
            local = block_rows(b)
            for i, target, column in (
                (1, in_pair_ref, second), (0, in_pair_ref, first),
                (2, in_grad_ref, first), (3, in_grad_ref, second),
            ):
                wait_bytes(rx.at[i, rows], m_recv.at[i, b + own_blocks])
                target[local, column] = rx[i, rows].astype(target.dtype)
            return carry

        lax.fori_loop(0, own_blocks, collect, 0)
        puts[2].start()
        puts[3].start()
        for a, cols, slot in (ways[0], ways[2], ways[1]):
            wait_bytes(result_rx.at[a, :, cols], e_recv.at[slot])
            results[(0, 2, 1)[slot]].start()

    @pl.when(is_mate)
    def _():
        wait_bytes(gain_parts.at[pl.ds(0, m)], c_recv)

    if m > 1:
        @pl.when(is_host)
        def _():
            wait_bytes(gain_parts.at[pl.ds(0, m - 1)], c_recv)

    total = gain_parts[0]
    for j in range(1, m):
        total = total + gain_parts[j]
    gain_out[...] = total

    @pl.when(is_host)
    def _():
        wait_bytes(gain_parts.at[pl.ds(0, n - 1)], c_send)
        for a, cols, slot in ways:
            wait_bytes(result_tx.at[a, :, cols], e_send.at[slot])
            if m > 1:
                if slot != 1:
                    wait_bytes(norms.at[a, pl.ds(0, 2), pl.ds(0, m - 1)], n_send.at[a])
                if slot == 0:
                    @pl.when(jnp.logical_not(routed))
                    def _():
                        wait_bytes(deltas.at[0, pl.ds(0, m - 1), whole, left], d_send.at[0])
                else:
                    wait_bytes(deltas.at[a, pl.ds(0, m - 1), whole, cols], d_send.at[slot])

        @pl.when(routed)
        def _():
            wait_bytes(delta_via, d_send.at[0])

        @pl.when(high)
        def _():
            wait_bytes(via, v_send.at[0])
            wait_bytes(g_via, v_send.at[1])

        if m > 1:
            @pl.when(routes)
            def _():
                for k in range(m - 1):
                    wait_bytes(delta_via, y_send)

        wait_bytes(tx.at[:, pl.ds(0, tokens)], m_send)

        @pl.when(has_below)
        def _():
            wait_bytes(tx, p_send)

    @pl.when(both(is_mate, low))
    def _():
        passed_on()

    @pl.when(feeds)
    def _():
        wait_bytes(tx.at[:, pl.ds(0, tokens)], feed_send)

    for put in puts[2:]:
        put.wait()

    @pl.when(is_host)
    def _():
        for put in puts[:2]:
            put.wait()

    @pl.when(is_mate)
    def _():
        for result in results:
            result.wait()


def put(k, *refs):
    sources, targets, held, wide = refs[:k], refs[k:2 * k], refs[2 * k:3 * k], refs[3 * k]
    in_sem, out_sem = refs[3 * k + 1:]
    steps, widened = [], 0
    for i in range(k):
        rows = sources[i].shape[0]
        pieces = 2 if rows % 32 == 0 else 1
        grows = sources[i].dtype != targets[i].dtype
        for c in range(pieces):
            lines = pl.ds(c * (rows // pieces), rows // pieces)
            taken = pltpu.make_async_copy(
                sources[i].at[lines], held[i].at[lines], in_sem.at[i, c]
            )
            source = wide.at[widened, lines] if grows else held[i].at[lines]
            given = pltpu.make_async_copy(source, targets[i].at[lines], out_sem.at[i, c])
            steps.append((taken, given, (i, widened, lines) if grows else None))
        widened += int(grows)
    for taken, _, _ in steps:
        taken.start()
    for taken, given, grow in steps:
        taken.wait()
        if grow is not None:
            i, place, lines = grow
            wide[place, lines] = held[i][lines].astype(f32)
        given.start()
    for _, given, _ in steps:
        given.wait()


def shards(out_pair, out_grad, f_weight, g_weight, gains):
    n, sections = lax.axis_size("dp"), lax.axis_size("section")
    tokens, width = out_pair.shape
    h = width // 2
    part = f_weight.shape[1]
    blocks = 8
    m = n // 2
    rows_all = 2 * tokens
    split = h // 2
    vmem, anywhere = pl.BlockSpec(memory_space=pltpu.VMEM), pl.BlockSpec(memory_space=pl.ANY)
    dma = pltpu.SemaphoreType.DMA
    outs = pl.pallas_call(
        functools.partial(kernel, n, sections, blocks),
        out_shape=(
            jax.ShapeDtypeStruct((tokens, width), f32),
            jax.ShapeDtypeStruct((tokens, width), bf16),
            jax.ShapeDtypeStruct((part, h), bf16),
            jax.ShapeDtypeStruct((part, h), bf16),
            jax.ShapeDtypeStruct((2, h), f32),
        ),
        in_specs=[anywhere] * 5,
        out_specs=[anywhere] * 4 + [vmem],
        scratch_shapes=[
            pltpu.VMEM((tokens, width), f32),
            pltpu.VMEM((tokens, width), bf16),
            pltpu.VMEM((part, h), bf16),
            pltpu.VMEM((part, h), bf16),
            pltpu.VMEM((2, h), f32),
            pltpu.VMEM((tokens, width), f32),
            pltpu.VMEM((tokens, width), bf16),
            pltpu.VMEM((part, h), bf16),
            pltpu.VMEM((part, h), bf16),
            pltpu.VMEM((h, h), bf16),
            pltpu.VMEM((h, h), bf16),
            pltpu.VMEM((h, h), bf16),
            pltpu.VMEM((h, h), bf16),
            pltpu.VMEM((2, part, h), bf16),
            pltpu.VMEM((4, rows_all, h), bf16),
            pltpu.VMEM((4, rows_all, h), bf16),
            pltpu.VMEM((4, rows_all // blocks, h), f32),
            pltpu.VMEM((2, rows_all // blocks, h), f32),
            pltpu.VMEM((2, n, rows_all, part), bf16),
            pltpu.VMEM((2, 2, m, rows_all, part), bf16),
            pltpu.VMEM((2, m, rows_all, h), bf16),
            pltpu.VMEM((2, part, h), bf16),
            pltpu.VMEM((2, part, h), bf16),
            pltpu.VMEM((2, h), f32),
            pltpu.VMEM((n, 2, h), f32),
            pltpu.VMEM((part, split), bf16),
            pltpu.VMEM((rows_all, split), bf16),
            pltpu.VMEM((part // 4, h), bf16),
            pltpu.SemaphoreType.REGULAR,
            pltpu.SemaphoreType.REGULAR,
            dma((2,)),
            dma((2,)),
            dma,
            dma((2, 4)),
            dma,
            dma,
            dma((4, blocks)),
            dma,
            dma((4, blocks)),
            dma((2,)),
            dma((2,)),
            dma((3,)),
            dma((3,)),
            dma,
            dma,
            dma((3,)),
            dma((3,)),
            dma((2,)),
            dma((3,)),
            dma,
            dma((blocks,)),
            dma((5,)),
            dma((5,)),
        ],
        compiler_params=pltpu.CompilerParams(
            collective_id=0, has_side_effects=True, vmem_limit_bytes=60 * 1024 * 1024
        ),
    )(out_pair, out_grad, f_weight[0], g_weight[0], gains[0])
    outs = pl.pallas_call(
        functools.partial(put, len(outs)),
        out_shape=tuple(
            jax.ShapeDtypeStruct(out.shape, bf16 if i == 1 else f32) for i, out in enumerate(outs)
        ),
        in_specs=[anywhere] * len(outs),
        out_specs=[anywhere] * len(outs),
        scratch_shapes=[
            *(pltpu.VMEM(out.shape, out.dtype) for out in outs),
            pltpu.VMEM((2, part, h), f32),
            dma((len(outs), 2)),
            dma((len(outs), 2)),
        ],
        compiler_params=pltpu.CompilerParams(vmem_limit_bytes=60 * 1024 * 1024),
    )(*outs)
    return tuple(out[None] for out in outs)


def solution(mesh):
    placed = (
        P("dp", None),
        P("dp", None),
        P("section", "dp", None),
        P("section", "dp", None),
        P("section", None, None),
    )
    return jax.shard_map(
        shards,
        mesh=mesh,
        in_specs=placed,
        out_specs=(
            P("section", "dp", None),
            P("section", "dp", None),
            P("section", "dp", None),
            P("section", "dp", None),
            P("section", None, None),
        ),
        check_vma=False,
    )
```

```python
import functools

import jax
import jax.numpy as jnp
from jax import lax
from jax.experimental import pallas as pl
from jax.experimental.pallas import tpu as pltpu
from jax.sharding import PartitionSpec as P

offset = 0.25
MESH = pl.DeviceIdType.MESH
f32, bf16 = jnp.float32, jnp.bfloat16


def silu_parts(pre_values):
    sigmoid_value = jax.nn.sigmoid(pre_values)
    return (pre_values * sigmoid_value, sigmoid_value * (1.0 + pre_values * (1.0 - sigmoid_value)))


def inverse_scale(values):
    return lax.rsqrt(jnp.mean(values * values, axis=-1, keepdims=True) + offset)


def kernel(
    n, sections, blocks,
    pair_in, grad_in, fw_in, gw_in, gains_in,
    in_pair_out, in_grad_out, f_put, g_put, gain_out,
    pair_ref, grad_ref, fw_ref, gw_ref, gains_ref, in_pair_ref, in_grad_ref, f_out, g_out,
    wf, wg, wft, wgt, relay, rx, tx, held, slopes, norms_own, norms, deltas, result_tx, result_rx, gain_acc, gain_parts, via, delta_via, g_via,
    go_sem, clear_sem, w_send, w_recv, r_send, r_recv, feed_send,
    p_send, p_recv, m_send, m_recv, n_send, n_recv, d_send, d_recv, c_send, c_recv, e_send, e_recv, v_send, v_recv, y_send, y_recv, l_sem, o_sem,
):
    s, d = lax.axis_index("section"), lax.axis_index("dp")
    loads = [
        pltpu.make_async_copy(source, target, l_sem.at[i])
        for i, (source, target) in enumerate((
            (gw_in, gw_ref), (fw_in, fw_ref), (pair_in, pair_ref), (grad_in, grad_ref),
            (gains_in, gains_ref),
        ))
    ]
    for load in loads:
        load.start()
    puts = [
        pltpu.make_async_copy(source, target, o_sem.at[i])
        for i, (source, target) in enumerate((
            (f_out, f_put), (g_out, g_put), (in_pair_ref, in_pair_out), (in_grad_ref, in_grad_out),
        ))
    ]
    split = via.shape[1]
    results = [
        pltpu.make_async_copy(result_rx.at[a, :, cols], target.at[:, cols], o_sem.at[slot])
        for a, target, cols, slot in (
            (0, f_put, pl.ds(0, split), 0),
            (1, g_put, pl.ds(0, g_put.shape[1]), 1),
            (0, f_put, pl.ds(split, f_put.shape[1] - split), 4),
        )
    ]
    m = n // 2
    half = sections // 2
    tokens = pair_ref.shape[0]
    h = pair_ref.shape[1] // 2
    part = fw_ref.shape[0]
    rows_all = 2 * tokens
    rows_per = rows_all // blocks
    own_blocks = blocks // 2

    pair_index = lax.div(d, 2)
    parity = lax.rem(pair_index, 2)
    host, mate = 2 * pair_index + 1 - parity, 2 * pair_index + parity
    is_host, is_mate = d == host, d == mate
    hosts = [2 * j + 1 - j % 2 for j in range(m)]

    is_last = s == sections - 1
    has_below = s > 0
    not_last = jnp.logical_not(is_last)
    partner = lax.rem(s + half, sections)
    high, low = s >= half, s < half
    both = jnp.logical_and

    chained = half % 2 == 0
    odd = lax.rem(s, 2) == 1
    even = jnp.logical_not(odd)
    follows = jnp.logical_not(both(odd, high))
    splits = both(even, high)
    halves = both(even, low)
    early = both(splits, s < sections - 2)
    waits = both(high, s >= sections - 2) if chained else high
    holds = jnp.logical_not(waits) & (high | both(odd, s > 1))
    routed = s < 2
    routes = both(high, s - half < 2)
    feeder = max(sections - 3, 0)
    feeds = both(s == feeder, is_mate)
    is_fed = both(is_last, is_host)

    barrier = pltpu.get_barrier_semaphore()

    def greet(section, replica):
        pl.semaphore_signal(barrier, inc=1, device_id=(section, replica), device_id_type=MESH)

    for k in range(1, n):
        greet(s, lax.rem(d + k, n))
    for k in range(n):
        greet(partner, lax.rem(d + k, n))

    @pl.when(has_below)
    def _():
        greet(s - 1, d)

    @pl.when(not_last)
    def _():
        greet(s + 1, d)

    @pl.when(feeds)
    def _():
        greet(sections - 1, host)

    @pl.when(is_fed)
    def _():
        greet(feeder, mate)

    neighbours = 2 * n - 1 + has_below.astype(jnp.int32) + not_last.astype(jnp.int32)
    neighbours += feeds.astype(jnp.int32) + is_fed.astype(jnp.int32)
    if chained:
        @pl.when(splits)
        def _():
            greet(s - half + 1, d)

        @pl.when(both(odd, low))
        def _():
            greet(s + half - 1, d)

        neighbours += (splits | both(odd, low)).astype(jnp.int32)

        @pl.when(both(high, both(even, is_mate)))
        def _():
            greet(s + 1, host)

        @pl.when(both(high, both(odd, is_host)))
        def _():
            greet(s - 1, mate)

        neighbours += both(high, both(even, is_mate) | both(odd, is_host)).astype(jnp.int32)
    for load in loads:
        load.wait()
    pl.semaphore_wait(barrier, neighbours)

    fulls, owns = (wf, wg), (fw_ref, gw_ref)
    order = (1, 0)
    pieces = 4
    first, second = pl.ds(0, h), pl.ds(h, h)
    every = pl.ds(0, h)

    def wait_bytes(ref, sem):
        pltpu.make_async_copy(ref, ref, sem).wait()

    def send(src, dst, send_sem, recv_sem, section, replica):
        pltpu.make_async_remote_copy(
            src_ref=src, dst_ref=dst, send_sem=send_sem, recv_sem=recv_sem,
            device_id=(section, replica), device_id_type=MESH,
        ).start()

    def shard(a, owner, lead=0, size=part):
        start = pl.multiple_of(owner * part, part) + lead
        return fulls[a].at[pl.ds(pl.multiple_of(start, size), size)]

    def block_rows(b):
        return pl.ds(pl.multiple_of(b * rows_per, rows_per), rows_per)

    def place_of(b):
        later = jnp.where(b <= own_blocks, b - 1 + own_blocks, b - own_blocks)
        return jnp.where(b == 0, 0, later)

    def feed():
        for i, (source, column) in enumerate(
            ((pair_ref, first), (pair_ref, second), (grad_ref, first), (grad_ref, second))
        ):
            tx[i, pl.ds(tokens, tokens)] = source[:, column].astype(bf16)
        for b in range(own_blocks, blocks):
            for i in (0, 1, 3, 2):
                rows = block_rows(b)
                send(
                    tx.at[i, rows], rx.at[i, rows], feed_send, p_recv.at[i, b],
                    sections - 1, host,
                )

    def go_low():
        go(s - half + 1)

    def go(section):
        pl.semaphore_signal(go_sem, inc=1, device_id=(section, d), device_id_type=MESH)

    def sent(a):
        if chained:
            @pl.when(early if a == order[0] else both(splits, jnp.logical_not(early)))
            def _():
                go_low()

            if a == order[1]:
                @pl.when(odd)
                def _():
                    go(s - 1)

    def weights_out():
        if chained:
            @pl.when(follows)
            def _():
                pl.semaphore_wait(go_sem, 1)

        @pl.when(is_host)
        def _():
            for a in order:
                for t in hosts:
                    @pl.when(d != t)
                    def _():
                        send(owns[a], shard(a, d), w_send.at[a], w_recv.at[a], s, t)
            for a in order:
                fulls[a][pl.ds(pl.multiple_of(d * part, part), part), :] = owns[a][...]
            for a in order:
                if m > 1:
                    wait_bytes(fulls[a].at[pl.ds(0, (m - 1) * part)], w_send.at[a])
                sent(a)

        @pl.when(is_mate)
        def _():
            for a in order:
                if m > 1:
                    size = part // pieces
                    for c in range(pieces):
                        rows = pl.ds(c * size, size)
                        relayed = True if c < pieces // 2 else jnp.logical_not(halves)

                        @pl.when(relayed)
                        def _():
                            send(
                                owns[a].at[rows], relay.at[a, rows], w_send.at[a],
                                r_recv.at[a, c], partner, d,
                            )
                send(owns[a], shard(a, d), w_send.at[a], w_recv.at[a], s, host)
                if m > 1:
                    @pl.when(halves)
                    def _():
                        lead = part // 2
                        for t in hosts:
                            @pl.when(host != t)
                            def _():
                                send(
                                    owns[a].at[pl.ds(lead, lead)], shard(a, d, lead, lead),
                                    w_send.at[a], w_recv.at[a], s, t,
                                )
            for a in order:
                if m > 1:
                    @pl.when(halves)
                    def _():
                        lead = part // 2
                        wait_bytes(fulls[a].at[pl.ds(0, part + m * lead)], w_send.at[a])

                    @pl.when(jnp.logical_not(halves))
                    def _():
                        wait_bytes(fulls[a].at[pl.ds(0, 2 * part)], w_send.at[a])
                else:
                    wait_bytes(fulls[a].at[pl.ds(0, part)], w_send.at[a])
                sent(a)

    def pass_on():
        if m > 1:
            size = part // pieces
            for a in order:
                for c in range(pieces):
                    rows = pl.ds(c * size, size)
                    relayed = True if c < pieces // 2 else jnp.logical_not(splits)

                    @pl.when(relayed)
                    def _():
                        wait_bytes(relay.at[a, rows], r_recv.at[a, c])
                        for t in hosts:
                            @pl.when(host != t)
                            def _():
                                send(
                                    relay.at[a, rows], shard(a, d, c * size, size), r_send,
                                    w_recv.at[a], partner, t,
                                )

    def passed_on():
        if m > 1:
            @pl.when(splits)
            def _():
                for k in range(m - 1):
                    wait_bytes(relay.at[0], r_send)

            @pl.when(jnp.logical_not(splits))
            def _():
                for k in range(m - 1):
                    wait_bytes(relay, r_send)

    def clear(section):
        pl.semaphore_signal(clear_sem, inc=1, device_id=(section, host), device_id_type=MESH)

    @pl.when(both(is_mate, low))
    def _():
        pass_on()

    weights_out()

    @pl.when(feeds)
    def _():
        feed()

    @pl.when(both(is_mate, high))
    def _():
        pass_on()
        passed_on()

        if chained:
            @pl.when(both(even, s >= sections - 2))
            def _():
                clear(s)
                clear(s + 1)
        else:
            clear(s)

    def take(i, b, rows, source, column):
        local = both(is_last, b < own_blocks)

        @pl.when(local)
        def _():
            held[i] = source[rows, column].astype(f32)

        @pl.when(jnp.logical_not(local))
        def _():
            wait_bytes(rx.at[i, rows], p_recv.at[i, b])
            held[i] = rx[i, rows].astype(f32)

    def give(i, b, rows, values):
        tx[i, rows] = values.astype(bf16)

        @pl.when(has_below)
        def _():
            send(tx.at[i, rows], rx.at[i, rows], p_send, p_recv.at[i, b], s - 1, d)

        @pl.when(b >= own_blocks)
        def _():
            send(tx.at[i, rows], rx.at[i, rows], m_send, m_recv.at[i, b], s, mate)

    def share_norm(a, rows):
        for j, t in enumerate(hosts):
            @pl.when(d != t)
            def _():
                send(
                    norms_own.at[a, pl.ds(2 * j, 2), rows],
                    norms.at[a, pl.ds(0, 2), pair_index, rows],
                    n_send.at[a], n_recv.at[a], s, t,
                )

    def share_delta(a, rows, cols, slot):
        for t in hosts:
            @pl.when(d != t)
            def _():
                send(
                    deltas.at[a, pair_index, rows, cols], deltas.at[a, pair_index, rows, cols],
                    d_send.at[slot], d_recv.at[slot], s, t,
                )

    left = pl.ds(0, via.shape[1])
    ways = ((1, every, 2), (0, left, 0), (0, pl.ds(left.size, h - left.size), 1))

    def route_delta(step, rows):
        send(
            deltas.at[0, pair_index, rows, left], delta_via.at[rows], d_send.at[0],
            y_recv.at[step], partner, host,
        )

    def forward(step, carry):
        rows = block_rows(place_of(step))
        wait_bytes(delta_via.at[rows], y_recv.at[step])
        for t in hosts:
            @pl.when(d != t)
            def _():
                send(
                    delta_via.at[rows], deltas.at[0, pair_index, rows, left],
                    y_send, d_recv.at[0], partner, t,
                )
        return carry

    def block(step, carry):
        b = place_of(step)
        rows = block_rows(b)
        is_own = b < own_blocks
        gain_f, gain_g = gains_ref[0:1, :], gains_ref[1:2, :]
        take(0, b, rows, pair_ref, first)
        y1 = held[0]
        r1 = inverse_scale(y1)
        norm_g = (y1 * r1 * gain_g).astype(bf16)
        pre_g = jnp.dot(norm_g, wg[...], preferred_element_type=f32)
        take(1, b, rows, pair_ref, second)
        act_g, slope_g = silu_parts(pre_g)
        x2 = held[1] - act_g
        give(1, b, rows, x2)
        held[1] = x2
        slopes[0] = slope_g

        @pl.when(is_own)
        def _():
            in_pair_ref[rows, second] = x2

        r2 = inverse_scale(x2)
        norm_f = (x2 * r2 * gain_f).astype(bf16)

        @pl.when(step == 0)
        def _():
            wait_bytes(wf.at[pl.ds(0, (n - 1) * part)], w_recv.at[0])

        pre_f = jnp.dot(norm_f, wf[...], preferred_element_type=f32)
        act_f, slope_f = silu_parts(pre_f)
        x1 = held[0] - act_f
        give(0, b, rows, x1)
        slopes[1] = slope_f

        @pl.when(is_own)
        def _():
            in_pair_ref[rows, first] = x1

        for e in range(n):
            norms_own[0, e, rows] = norm_f[:, e * part:(e + 1) * part]
            norms_own[1, e, rows] = norm_g[:, e * part:(e + 1) * part]

        streams = jnp.logical_not(waits | both(holds, step < blocks // 2))

        @pl.when(both(holds, step == blocks // 2))
        def _():
            for earlier in range(blocks // 2):
                place = 0 if earlier == 0 else earlier - 1 + own_blocks
                held_rows = pl.ds(place * rows_per, rows_per)
                share_norm(1, held_rows)
                share_delta(1, held_rows, every, 2)
                share_norm(0, held_rows)

        @pl.when(streams)
        def _():
            share_norm(1, rows)
            share_norm(0, rows)

        @pl.when(step == 0)
        def _():
            wgt[...] = wg[...].T
            wft[...] = wf[...].T

        take(3, b, rows, grad_ref, second)
        take(2, b, rows, grad_ref, first)
        delta_g = (held[3] * slopes[0]).astype(bf16)
        back_g = jnp.dot(delta_g, wgt[...], preferred_element_type=f32)
        deltas[1, pair_index, rows] = delta_g

        @pl.when(streams)
        def _():
            share_delta(1, rows, every, 2)

        y1 = held[0]
        weighted = gain_g * back_g
        gz = held[2] + r1 * weighted - y1 * (r1 * r1 * r1) * jnp.mean(
            weighted * y1, axis=-1, keepdims=True
        )
        give(2, b, rows, gz)

        @pl.when(is_own)
        def _():
            in_grad_ref[rows, first] = gz.astype(bf16)

        gain_acc[1:2, :] += jnp.sum(back_g * y1 * r1, axis=0, keepdims=True)
        delta_f = (gz * slopes[1]).astype(bf16)
        back_f = jnp.dot(delta_f, wft[...], preferred_element_type=f32)
        deltas[0, pair_index, rows] = delta_f

        @pl.when(routed)
        def _():
            route_delta(step, rows)

        x2 = held[1]
        weighted = gain_f * back_f
        gx2 = held[3] + r2 * weighted - x2 * (r2 * r2 * r2) * jnp.mean(
            weighted * x2, axis=-1, keepdims=True
        )
        give(3, b, rows, gx2)

        @pl.when(is_own)
        def _():
            in_grad_ref[rows, second] = gx2.astype(bf16)

        gain_acc[0:1, :] += jnp.sum(back_f * x2 * r2, axis=0, keepdims=True)
        return carry

    whole = pl.ds(0, rows_all)
    outs = (f_out, g_out)

    def product(a, which, cols):
        return lax.dot_general(
            norms[a, which].reshape(m * rows_all, part),
            deltas[a, :, :, cols].reshape(m * rows_all, cols.size),
            (((0,), (0,)), ((), ())), preferred_element_type=f32,
        )

    @pl.when(is_host)
    def _():
        gain_acc[...] = jnp.zeros_like(gain_acc)
        wait_bytes(wg.at[pl.ds(0, (n - 1) * part)], w_recv.at[1])
        lax.fori_loop(0, blocks, block, 0)
        puts[2].start()
        puts[3].start()

        @pl.when(waits)
        def _():
            pl.semaphore_wait(clear_sem, 1)
            share_norm(1, whole)
            share_delta(*ways[0][:1], whole, *ways[0][1:])
            share_norm(0, whole)
            for a, cols, slot in ways[1:]:
                share_delta(a, whole, cols, slot)

        @pl.when(jnp.logical_not(waits | routed))
        def _():
            share_delta(*ways[1][:1], whole, *ways[1][1:])

        @pl.when(jnp.logical_not(waits))
        def _():
            share_delta(*ways[2][:1], whole, *ways[2][1:])

        gain_parts[pair_index] = gain_acc[...]
        for k in range(1, n):
            send(
                gain_parts.at[pair_index], gain_parts.at[pair_index], c_send, c_recv,
                s, lax.rem(d + k, n),
            )
        for a in range(2):
            for w in range(2):
                norms[a, w, pair_index] = norms_own[a, 2 * pair_index + w]
        for a, cols, slot in ways:
            if m > 1:
                if slot != 1:
                    wait_bytes(norms.at[a, pl.ds(0, 2), pl.ds(0, m - 1)], n_recv.at[a])
                wait_bytes(deltas.at[a, pl.ds(0, m - 1), whole, cols], d_recv.at[slot])
            result_tx[a, :, cols] = product(a, parity, cols).astype(bf16)

            def direct():
                send(
                    result_tx.at[a, :, cols], result_rx.at[a, :, cols], e_send.at[slot],
                    e_recv.at[slot], s, mate,
                )

            if slot == 2:
                head, end = pl.ds(0, part - g_via.shape[0]), pl.ds(part - g_via.shape[0], g_via.shape[0])
                send(
                    result_tx.at[1, head], result_rx.at[1, head], e_send.at[slot],
                    e_recv.at[slot], s, mate,
                )

                @pl.when(high)
                def _():
                    send(
                        result_tx.at[1, end], result_rx.at[1, end], e_send.at[slot],
                        e_recv.at[slot], s, mate,
                    )

                @pl.when(low)
                def _():
                    send(
                        result_tx.at[1, end], g_via, e_send.at[slot], v_recv.at[2],
                        partner, host,
                    )
            elif slot == 0:
                @pl.when(high)
                def _():
                    direct()

                @pl.when(low)
                def _():
                    for c in range(2):
                        lines = pl.ds(c * (part // 2), part // 2)
                        send(
                            result_tx.at[a, lines, cols], via.at[lines], e_send.at[slot],
                            v_recv.at[c], partner, host,
                        )
            else:
                direct()
        @pl.when(routes)
        def _():
            lax.fori_loop(0, blocks, forward, 0)

        for a in order:
            outs[a][...] = product(a, 1 - parity, every).astype(bf16)
            puts[a].start()

        @pl.when(high)
        def _():
            wait_bytes(g_via, v_recv.at[2])
            end = pl.ds(part - g_via.shape[0], g_via.shape[0])
            send(g_via, result_rx.at[1, end], v_send.at[1], e_recv.at[2], partner, mate)
            for c in range(2):
                lines = pl.ds(c * (part // 2), part // 2)
                wait_bytes(via.at[lines], v_recv.at[c])
                send(
                    via.at[lines], result_rx.at[0, lines, left], v_send.at[0], e_recv.at[0],
                    partner, mate,
                )

    @pl.when(is_mate)
    def _():
        def collect(b, carry):
            rows = block_rows(b + own_blocks)
            local = block_rows(b)
            for i, target, column in (
                (1, in_pair_ref, second), (0, in_pair_ref, first),
                (2, in_grad_ref, first), (3, in_grad_ref, second),
            ):
                wait_bytes(rx.at[i, rows], m_recv.at[i, b + own_blocks])
                target[local, column] = rx[i, rows].astype(target.dtype)
            return carry

        lax.fori_loop(0, own_blocks, collect, 0)
        puts[2].start()
        puts[3].start()
        for a, cols, slot in (ways[0], ways[2], ways[1]):
            wait_bytes(result_rx.at[a, :, cols], e_recv.at[slot])
            results[(0, 2, 1)[slot]].start()

    @pl.when(is_mate)
    def _():
        wait_bytes(gain_parts.at[pl.ds(0, m)], c_recv)

    if m > 1:
        @pl.when(is_host)
        def _():
            wait_bytes(gain_parts.at[pl.ds(0, m - 1)], c_recv)

    total = gain_parts[0]
    for j in range(1, m):
        total = total + gain_parts[j]
    gain_out[...] = total

    @pl.when(is_host)
    def _():
        wait_bytes(gain_parts.at[pl.ds(0, n - 1)], c_send)
        for a, cols, slot in ways:
            wait_bytes(result_tx.at[a, :, cols], e_send.at[slot])
            if m > 1:
                if slot != 1:
                    wait_bytes(norms.at[a, pl.ds(0, 2), pl.ds(0, m - 1)], n_send.at[a])
                if slot == 0:
                    @pl.when(jnp.logical_not(routed))
                    def _():
                        wait_bytes(deltas.at[0, pl.ds(0, m - 1), whole, left], d_send.at[0])
                else:
                    wait_bytes(deltas.at[a, pl.ds(0, m - 1), whole, cols], d_send.at[slot])

        @pl.when(routed)
        def _():
            wait_bytes(delta_via, d_send.at[0])

        @pl.when(high)
        def _():
            wait_bytes(via, v_send.at[0])
            wait_bytes(g_via, v_send.at[1])

        if m > 1:
            @pl.when(routes)
            def _():
                for k in range(m - 1):
                    wait_bytes(delta_via, y_send)

        wait_bytes(tx.at[:, pl.ds(0, tokens)], m_send)

        @pl.when(has_below)
        def _():
            wait_bytes(tx, p_send)

    @pl.when(both(is_mate, low))
    def _():
        passed_on()

    @pl.when(feeds)
    def _():
        wait_bytes(tx.at[:, pl.ds(0, tokens)], feed_send)

    for put in puts[2:]:
        put.wait()

    @pl.when(is_host)
    def _():
        for put in puts[:2]:
            put.wait()

    @pl.when(is_mate)
    def _():
        for result in results:
            result.wait()


def put(k, *refs):
    sources, targets, held, wide = refs[:k], refs[k:2 * k], refs[2 * k:3 * k], refs[3 * k]
    in_sem, out_sem = refs[3 * k + 1:]
    steps, widened = [], 0
    for i in range(k):
        rows = sources[i].shape[0]
        pieces = 2 if rows % 32 == 0 else 1
        grows = sources[i].dtype != targets[i].dtype
        for c in range(pieces):
            lines = pl.ds(c * (rows // pieces), rows // pieces)
            taken = pltpu.make_async_copy(
                sources[i].at[lines], held[i].at[lines], in_sem.at[i, c]
            )
            source = wide.at[widened, lines] if grows else held[i].at[lines]
            given = pltpu.make_async_copy(source, targets[i].at[lines], out_sem.at[i, c])
            steps.append((taken, given, (i, widened, lines) if grows else None))
        widened += int(grows)
    for taken, _, _ in steps:
        taken.start()
    for taken, given, grow in steps:
        taken.wait()
        if grow is not None:
            i, place, lines = grow
            wide[place, lines] = held[i][lines].astype(f32)
        given.start()
    for _, given, _ in steps:
        given.wait()


def shards(out_pair, out_grad, f_weight, g_weight, gains):
    n, sections = lax.axis_size("dp"), lax.axis_size("section")
    tokens, width = out_pair.shape
    h = width // 2
    part = f_weight.shape[1]
    blocks = 8
    m = n // 2
    rows_all = 2 * tokens
    split = h // 2
    vmem, anywhere = pl.BlockSpec(memory_space=pltpu.VMEM), pl.BlockSpec(memory_space=pl.ANY)
    dma = pltpu.SemaphoreType.DMA
    outs = pl.pallas_call(
        functools.partial(kernel, n, sections, blocks),
        out_shape=(
            jax.ShapeDtypeStruct((tokens, width), f32),
            jax.ShapeDtypeStruct((tokens, width), bf16),
            jax.ShapeDtypeStruct((part, h), bf16),
            jax.ShapeDtypeStruct((part, h), bf16),
            jax.ShapeDtypeStruct((2, h), f32),
        ),
        in_specs=[anywhere] * 5,
        out_specs=[anywhere] * 4 + [vmem],
        scratch_shapes=[
            pltpu.VMEM((tokens, width), f32),
            pltpu.VMEM((tokens, width), bf16),
            pltpu.VMEM((part, h), bf16),
            pltpu.VMEM((part, h), bf16),
            pltpu.VMEM((2, h), f32),
            pltpu.VMEM((tokens, width), f32),
            pltpu.VMEM((tokens, width), bf16),
            pltpu.VMEM((part, h), bf16),
            pltpu.VMEM((part, h), bf16),
            pltpu.VMEM((h, h), bf16),
            pltpu.VMEM((h, h), bf16),
            pltpu.VMEM((h, h), bf16),
            pltpu.VMEM((h, h), bf16),
            pltpu.VMEM((2, part, h), bf16),
            pltpu.VMEM((4, rows_all, h), bf16),
            pltpu.VMEM((4, rows_all, h), bf16),
            pltpu.VMEM((4, rows_all // blocks, h), f32),
            pltpu.VMEM((2, rows_all // blocks, h), f32),
            pltpu.VMEM((2, n, rows_all, part), bf16),
            pltpu.VMEM((2, 2, m, rows_all, part), bf16),
            pltpu.VMEM((2, m, rows_all, h), bf16),
            pltpu.VMEM((2, part, h), bf16),
            pltpu.VMEM((2, part, h), bf16),
            pltpu.VMEM((2, h), f32),
            pltpu.VMEM((n, 2, h), f32),
            pltpu.VMEM((part, split), bf16),
            pltpu.VMEM((rows_all, split), bf16),
            pltpu.VMEM((part // 4, h), bf16),
            pltpu.SemaphoreType.REGULAR,
            pltpu.SemaphoreType.REGULAR,
            dma((2,)),
            dma((2,)),
            dma,
            dma((2, 4)),
            dma,
            dma,
            dma((4, blocks)),
            dma,
            dma((4, blocks)),
            dma((2,)),
            dma((2,)),
            dma((3,)),
            dma((3,)),
            dma,
            dma,
            dma((3,)),
            dma((3,)),
            dma((2,)),
            dma((3,)),
            dma,
            dma((blocks,)),
            dma((5,)),
            dma((5,)),
        ],
        compiler_params=pltpu.CompilerParams(
            collective_id=0, has_side_effects=True, vmem_limit_bytes=60 * 1024 * 1024
        ),
    )(out_pair, out_grad, f_weight[0], g_weight[0], gains[0])
    outs = pl.pallas_call(
        functools.partial(put, len(outs)),
        out_shape=tuple(
            jax.ShapeDtypeStruct(out.shape, bf16 if i == 1 else f32) for i, out in enumerate(outs)
        ),
        in_specs=[anywhere] * len(outs),
        out_specs=[anywhere] * len(outs),
        scratch_shapes=[
            *(pltpu.VMEM(out.shape, out.dtype) for out in outs),
            pltpu.VMEM((2, part, h), f32),
            dma((len(outs), 2)),
            dma((len(outs), 2)),
        ],
        compiler_params=pltpu.CompilerParams(vmem_limit_bytes=60 * 1024 * 1024),
    )(*outs)
    return tuple(out[None] for out in outs)


def solution(mesh):
    placed = (
        P("dp", None),
        P("dp", None),
        P("section", "dp", None),
        P("section", "dp", None),
        P("section", None, None),
    )
    return jax.shard_map(
        shards,
        mesh=mesh,
        in_specs=placed,
        out_specs=(
            P("section", "dp", None),
            P("section", "dp", None),
            P("section", "dp", None),
            P("section", "dp", None),
            P("section", None, None),
        ),
        check_vma=False,
    )
```
